128 devices in a mesh: blk: 32 (over x, z_lo, y), table: 4 (over z_hi, core).
Axes of the slice: x: 4, y: 4, z: 4 (z_hi: 2, z_lo: 2; z = z_hi * 2 + z_lo), core: 2. Of those that a mesh axis runs over, the one named last changes fastest.
Arguments:
- queries: bfloat16 [65536, 256], P(('blk', 'table')), may hold values from -20 to 20
- items: bfloat16 [65536, 256], P(('blk', 'table')), may hold values from -4.8 to 4.8
- positives: int32 [65536], P(('blk', 'table')), may hold values from 0 to 511
- item_owner: int32 [65536, 1], P(('blk', 'table')), may hold values from 0 to 127; in each aligned block of 512 rows (0 to 511, 512 to 1023, ...) at most 12 rows name the same one
- item_row: int32 [65536], P(('blk', 'table')), may hold values from 0 to 16383
Outputs:
- query_grad: bfloat16 [65536, 256], P(('blk', 'table'))
- item_grad: bfloat16 [65536, 256], P(('blk', 'table'))
- table_grad: bfloat16 [2097152, 256], P(('blk', 'table'))
The draws below stay inside these ranges and needn't reach their ends.
Inputs may be any that keep to these rules, and one draw needn't show every extreme that they name: `item_owner`: among the rows of one device, no owner is named more than 12 times, a bound that some block reaches.
All inputs are finite; a program needn't handle non-finite values.
Results may differ from the reference program's by a relative error of at most 0.0034.
Values may be sent and summed in bfloat16 or wider, within the bound.
A program may use at most 64 MiB of HBM per device.

```python
import math
import jax
import jax.numpy as jnp
import numpy as np
from jax import lax

D = 256
ROWS_DEV = 16384
ITEMS_DEV = 512
WINDOW = 16
CAP = 12
BATCH = 65536
ROWS = 2097152
N_BLK = 32
N_TABLE = 4
DEVICES = 128


def pair_draw(key):
    query_key = jax.random.fold_in(key, 101)
    item_key = jax.random.fold_in(key, 102)
    items_base = jnp.clip(jax.random.normal(item_key, (BATCH, D), jnp.float32), -4.0, 4.0)
    query_base = jnp.clip(jax.random.normal(query_key, (BATCH, D), jnp.float32), -4.0, 4.0)
    return (query_base, items_base)


def draw_queries(key, part):
    return pair_draw(key)[0].astype(jnp.bfloat16)


def draw_items(key, part):
    return pair_draw(key)[1].astype(jnp.bfloat16)


def plant(values, key, low, high):
    longest = values.shape.index(max(values.shape))
    spots = []
    for shift in (0, 1):
        where = [jax.random.randint(jax.random.fold_in(key, axis), (), 0, length) for axis, length in enumerate(values.shape)]
        where[longest] = (where[longest] + shift) % values.shape[longest]
        spots.append(tuple(where))
    return values.at[spots[0]].set(low).at[spots[1]].set(high)


def shared_out(own_key, own, number, rows, number_of, top, limit, slope):
    sequence = jax.random.permutation(own_key, number_of)
    packed, ordinary = load_shares(number_of, rows * top, limit, slope, True), load_shares(number_of, rows * top, limit, slope, False)
    places = jnp.arange(number_of)

    def named(tallies, offset_by):
        used = int((tallies > 0).sum())
        fixed = max(1, used // 4)
        shifted = fixed + (places - fixed + offset_by * (used - fixed)) % max(1, number_of - fixed)
        return jnp.zeros((number_of,), jnp.int32).at[sequence[jnp.where(places < fixed, places, shifted)]].set(jnp.asarray(tallies, jnp.int32))

    tallies = jnp.where(number % 4 == 0, named(packed, number // 4), named(ordinary, number - number // 4 - 1))
    mixed = jax.random.permutation(jax.random.fold_in(own, 3), number_of)
    giver, taker = mixed[0:number_of // 2 * 2:2], mixed[1:number_of // 2 * 2:2]
    margin = jnp.minimum(tallies[giver] - 1, limit - tallies[taker]) // 2
    margin = jnp.where((giver == sequence[0]) | (taker == sequence[0]) | (tallies[taker] == 0), 0, jnp.maximum(margin, 0))
    shifted = jax.random.randint(jax.random.fold_in(own, 4), (number_of // 2,), 0, 1 << 20) % (margin + 1)
    tallies = tallies.at[giver].add(-shifted).at[taker].add(shifted)
    labels = jnp.searchsorted(jnp.cumsum(tallies), jnp.arange(rows * top), side="right").astype(jnp.int32)
    listing = labels.reshape(top, rows).T
    listing = listing[jax.random.permutation(jax.random.fold_in(own, 1), rows)]
    offset_by = jax.random.randint(jax.random.fold_in(own, 2), (rows, 1), 0, top)
    return jnp.take_along_axis(listing, (jnp.arange(top)[None, :] + offset_by) % top, axis=1)


def load_shares(amount, total, bound, skew, full):
    weights = [(1 << 20) // math.isqrt(grade ** skew) + 1 for grade in range(1, amount + 1)]
    largest = bound if full else min(bound, max(-(-total // amount), total * weights[0] // sum(weights)))
    least = 1 if total - largest >= amount - 1 else 0
    holding, spare = [largest] + [least] * (amount - 1), total - largest - least * (amount - 1)
    while spare > 0:
        candidates = [i for i in range(1, amount) if holding[i] < largest] or [i for i in range(1, amount) if holding[i] < bound]
        mass, budget = sum([weights[i] for i in candidates]), spare
        for i in candidates:
            more = min(bound - holding[i], max(1, budget * weights[i] // mass), spare)
            holding[i] = holding[i] + more
            spare = spare - more
    return np.array(holding)


def setup_inputs(seed: int = 0) -> dict:
    streams_of = jax.random.split(jax.random.key(seed), 6)
    queries = draw_queries(jax.random.fold_in(streams_of[5], 71), 0)
    items = draw_items(jax.random.fold_in(streams_of[5], 71), 0)
    positives = plant(jax.random.randint(streams_of[2], (BATCH,), 0, ITEMS_DEV), jax.random.fold_in(streams_of[2], 1), 0, ITEMS_DEV - 1).astype(jnp.int32)
    item_owner_keys = jax.random.split(jax.random.fold_in(streams_of[3], 1), BATCH // ITEMS_DEV)
    item_owner_turns = jax.random.permutation(jax.random.fold_in(streams_of[3], 3), BATCH // ITEMS_DEV)
    item_owner = jax.vmap(lambda own, number: shared_out(jax.random.fold_in(streams_of[3], 2), own, number, ITEMS_DEV, DEVICES, 1, CAP, 2))(item_owner_keys, item_owner_turns).reshape((BATCH, 1))
    item_row = plant(jax.random.randint(streams_of[4], (BATCH,), 0, ROWS_DEV), jax.random.fold_in(streams_of[4], 1), 0, ROWS_DEV - 1).astype(jnp.int32)
    return dict(queries=queries, items=items, positives=positives, item_owner=item_owner, item_row=item_row)


def reference(queries, items, positives, item_owner, item_row):
    feature_width = queries.shape[1]
    logit_scale = 3.0 / math.sqrt(feature_width)
    grid_shape = (N_BLK, N_TABLE, ITEMS_DEV, feature_width)
    query_all = queries.reshape(grid_shape)
    items_all = items.reshape(grid_shape)
    positive_all = positives.reshape(N_BLK, N_TABLE, ITEMS_DEV)
    places = jnp.arange(ITEMS_DEV, dtype=jnp.int32)
    block_ids = jnp.arange(N_BLK * N_TABLE, dtype=jnp.int32)

    def scores_of(query_block, item_block):
        return logit_scale * jnp.dot(query_block.astype(jnp.float32), item_block.astype(jnp.float32).T, precision=lax.Precision.HIGHEST)

    def fetch(grid, row_block, column):
        return lax.dynamic_index_in_dim(lax.dynamic_index_in_dim(grid, row_block, 0, keepdims=False), column, 0, keepdims=False)

    def totals_one(block_id):
        row_block = (block_id // N_TABLE).astype(jnp.int32)
        column = (block_id % N_TABLE).astype(jnp.int32)
        query_block = fetch(query_all, row_block, column)
        scores = scores_of(query_block, fetch(items_all, row_block, column))
        top_now = lax.optimization_barrier(jnp.max(scores, axis=1))
        total_now = lax.optimization_barrier(jnp.sum(jnp.exp(scores - top_now[:, None]), axis=1))
        for offset in range(1, WINDOW):
            source = ((row_block - offset) % N_BLK).astype(jnp.int32)
            scores = scores_of(query_block, fetch(items_all, source, column))
            top_new = jnp.maximum(top_now, lax.optimization_barrier(jnp.max(scores, axis=1)))
            total_now = total_now * jnp.exp(top_now - top_new) + lax.optimization_barrier(jnp.sum(jnp.exp(scores - top_new[:, None]), axis=1))
            top_now = top_new
        return top_now + jnp.log(total_now)
    log_total = lax.map(totals_one, block_ids).reshape(N_BLK, N_TABLE, ITEMS_DEV)

    def weights_of(query_block, item_block, totals, positive_rows, offset):
        weights = jnp.exp(scores_of(query_block, item_block) - totals[:, None])
        if offset == 0:
            weights = weights - (positive_rows[:, None] == places[None, :]).astype(weights.dtype)
        return lax.optimization_barrier(weights.astype(jnp.bfloat16)).astype(jnp.float32)

    def query_side(block_id):
        row_block = (block_id // N_TABLE).astype(jnp.int32)
        column = (block_id % N_TABLE).astype(jnp.int32)
        query_block = fetch(query_all, row_block, column)
        totals = fetch(log_total, row_block, column)
        positive_rows = fetch(positive_all, row_block, column)
        summed = jnp.zeros((ITEMS_DEV, feature_width), jnp.float32)
        for offset in range(WINDOW):
            source = ((row_block - offset) % N_BLK).astype(jnp.int32)
            item_block = fetch(items_all, source, column)
            weights = weights_of(query_block, item_block, totals, positive_rows, offset)
            summed = summed + jnp.dot(weights, item_block.astype(jnp.float32), precision=lax.Precision.HIGHEST)
        return (logit_scale * summed).astype(jnp.bfloat16)

    def item_side(block_id):
        row_block = (block_id // N_TABLE).astype(jnp.int32)
        column = (block_id % N_TABLE).astype(jnp.int32)
        item_block = fetch(items_all, row_block, column)
        summed = jnp.zeros((ITEMS_DEV, feature_width), jnp.float32)
        for offset in range(WINDOW):
            target = ((row_block + offset) % N_BLK).astype(jnp.int32)
            query_block = fetch(query_all, target, column)
            weights = weights_of(query_block, item_block, fetch(log_total, target, column), fetch(positive_all, target, column), offset)
            summed = summed + jnp.dot(weights.T, query_block.astype(jnp.float32), precision=lax.Precision.HIGHEST)
        return (logit_scale * summed).astype(jnp.bfloat16)
    query_grad = lax.map(query_side, block_ids).reshape(BATCH, feature_width)
    item_grad = lax.map(item_side, block_ids).reshape(BATCH, feature_width)
    grad_rows = item_grad.astype(jnp.float32)
    owners = item_owner[:, 0]

    def one_owner(owner):
        target = jnp.where(owners == owner, item_row, ROWS_DEV).astype(jnp.int32)
        summed = jnp.zeros((ROWS_DEV, feature_width), jnp.float32).at[target].add(grad_rows, mode='drop')
        return summed.astype(jnp.bfloat16)
    table_grad = lax.map(one_owner, jnp.arange(DEVICES, dtype=jnp.int32)).reshape(ROWS, feature_width)
    return (query_grad, item_grad, table_grad)
```

```python
import math

import jax
import jax.numpy as jnp
from jax import lax
from jax.experimental import pallas as pl
from jax.experimental.pallas import tpu as pltpu
from jax.sharding import PartitionSpec as P

ROWS_DEV = 16384
N = 512
D = 256
H = 256
SCALE = 3.0 / math.sqrt(D)
LOG2E = 1.4426950408889634
C2 = SCALE * LOG2E
MESH = pl.DeviceIdType.MESH
NT = (((1,), (1,)), ((), ()))
NN = (((1,), (0,)), ((), ()))
F32 = jnp.float32
BF16 = jnp.bfloat16


def main_kernel(
    q_hbm, k_hbm, pos_ref,
    dq_ref, dk_ref,
    qbuf, kbuf, sbuf, gbuf, kt, lk, lst, lse, acc, pk, pr, dqs, dqr,
    lsem, ssem, rsem, st_s, st_r, dq_s, dq_r,
):
    b = lax.axis_index("blk")
    x = b // 8
    me = b % 8
    z = me // 4
    y = me % 4

    def slot(r, s):
        return 4 * ((z + s) % 2) + (y + r) % 4

    def group(p):
        return {"blk": x * 8 + p}

    xp = {"blk": ((x + 1) % 4) * 8 + me}
    xm = {"blk": ((x + 3) % 4) * 8 + me}
    yp = group(slot(1, 0))
    ym = group(slot(3, 0))
    zp = group(slot(0, 1))

    own_q = pltpu.make_async_copy(q_hbm, qbuf.at[me], lsem.at[0])
    own_k = pltpu.make_async_copy(k_hbm, kbuf.at[0], lsem.at[1])
    own_q.start()
    own_k.start()

    barrier = pltpu.get_barrier_semaphore()
    for o in range(1, 8):
        pl.semaphore_signal(barrier, inc=1, device_id=group((me + o) % 8), device_id_type=MESH)
    for dev in (xp, xm):
        pl.semaphore_signal(barrier, inc=1, device_id=dev, device_id_type=MESH)
    pl.semaphore_wait(barrier, 9)
    own_k.wait()
    own_q.wait()

    def half(ref, i, c):
        return ref.at[i, pl.ds(c * H, H)]

    def send(n, src, dst, dev):
        copy = pltpu.make_async_remote_copy(
            src_ref=src, dst_ref=dst, send_sem=ssem.at[n], recv_sem=rsem.at[n],
            device_id=dev, device_id_type=MESH,
        )
        copy.start()
        return copy

    def arrived(n, ref):
        pltpu.make_async_remote_copy(
            src_ref=ref, dst_ref=ref, send_sem=ssem.at[n], recv_sem=rsem.at[n],
            device_id=xp, device_id_type=MESH,
        ).wait_recv()

    sent = []

    def k_send(n, i, j, c):
        sent.append(send(n, half(kbuf, i, c), half(kbuf, j, c), xp))

    def q_send(n, i, c, dev):
        sent.append(send(n, half(qbuf, i, c), half(qbuf, i, c), dev))

    k_send(0, 0, 1, 0)
    q_send(4, me, 0, yp)
    q_send(7, me, 1, ym)
    q_send(8, me, 0, zp)
    k_send(1, 0, 1, 1)
    q_send(5, me, 1, yp)
    q_send(6, me, 0, ym)
    q_send(9, me, 1, zp)

    def scores(qi, kind, ks):
        q = qbuf[qi]

        def tile(t, top):
            s = lax.dot_general(kbuf[ks, pl.ds(t * H, H), :], q, NT, preferred_element_type=F32)
            sbuf[kind, qi, pl.ds(t * H, H), :] = s
            return jnp.maximum(top, jnp.max(s.reshape(H // 8, 8, N), axis=0))

        top = lax.fori_loop(0, 2, tile, jnp.full((8, N), -jnp.inf, F32))
        top = jnp.max(top, axis=0, keepdims=True) * C2

        def tile2(t, total):
            s = sbuf[kind, qi, pl.ds(t * H, H), :]
            return total + jnp.sum(jnp.exp2(s * C2 - top).reshape(H // 8, 8, N), axis=0)

        total = lax.fori_loop(0, 2, tile2, jnp.zeros((8, N), F32))
        total = jnp.sum(total, axis=0, keepdims=True)
        lk[kind, pl.ds(qi, 1), :] = top + jnp.log(total) * LOG2E

    def mixed_k(qi):
        return jnp.where(qi >= me, 0, 2)

    scores(me, 1, 0)

    s3, s1, s2, s0 = slot(3, 0), slot(1, 0), slot(2, 0), slot(0, 1)
    t3, t1, t2 = slot(3, 1), slot(1, 1), slot(2, 1)
    arrived(0, half(kbuf, 1, 0))
    k_send(2, 1, 2, 0)
    arrived(4, half(qbuf, s3, 0))
    q_send(10, s3, 0, yp)
    arrived(7, half(qbuf, s1, 1))
    q_send(11, s1, 1, ym)
    arrived(8, half(qbuf, s0, 0))
    q_send(12, s0, 0, yp)
    q_send(14, s0, 0, ym)
    arrived(1, half(kbuf, 1, 1))
    k_send(3, 1, 2, 1)
    arrived(9, half(qbuf, s0, 1))
    q_send(13, s0, 1, yp)
    q_send(15, s0, 1, ym)
    arrived(5, half(qbuf, s3, 1))
    arrived(6, half(qbuf, s1, 0))
    scores(me, 0, 1)
    arrived(10, half(qbuf, s2, 0))
    q_send(16, s2, 0, zp)
    arrived(11, half(qbuf, s2, 1))
    q_send(17, s2, 1, zp)

    def first_full(j, carry):
        scores(slot(j, (4 - j) // 4), 0, 1)
        return carry

    lax.fori_loop(0, 4, first_full, 0)
    arrived(2, half(kbuf, 2, 0))
    arrived(3, half(kbuf, 2, 1))

    def turn(i, carry):
        kt[i] = kbuf[i].T
        return carry

    lax.fori_loop(0, 3, turn, 0)

    def first_mixed(j, carry):
        qi = slot(j, (4 - j) // 4)
        scores(qi, 1, mixed_k(qi))
        return carry

    lax.fori_loop(0, 4, first_mixed, 0)
    arrived(12, half(qbuf, t3, 0))
    arrived(14, half(qbuf, t1, 0))
    arrived(13, half(qbuf, t3, 1))
    arrived(15, half(qbuf, t1, 1))
    arrived(16, half(qbuf, t2, 0))
    arrived(17, half(qbuf, t2, 1))

    def last_pairs(j, carry):
        qi = slot(j, 1)
        scores(qi, 0, 1)
        scores(qi, 1, mixed_k(qi))
        return carry

    lax.fori_loop(1, 4, last_pairs, 0)

    a, c = lk[0], lk[1]
    top = jnp.maximum(a, c)
    lst[me] = top + jnp.log(jnp.exp2(a - top) + jnp.exp2(c - top)) * LOG2E
    stats = []
    for o in range(1, 8):
        copy = pltpu.make_async_remote_copy(
            src_ref=lst.at[me], dst_ref=lst.at[me], send_sem=st_s.at[o - 1], recv_sem=st_r.at[o - 1],
            device_id=group((me + o) % 8), device_id_type=MESH,
        )
        copy.start()
        stats.append(copy)
    for o in range(1, 8):
        p = (me + 8 - o) % 8
        pltpu.make_async_remote_copy(
            src_ref=lst.at[p], dst_ref=lst.at[p], send_sem=st_s.at[o - 1], recv_sem=st_r.at[o - 1],
            device_id=xp, device_id_type=MESH,
        ).wait_recv()
    top = lst[0]
    for i in range(1, 8):
        top = jnp.maximum(top, lst[i])
    total = jnp.exp2(lst[0] - top)
    for i in range(1, 8):
        total = total + jnp.exp2(lst[i] - top)
    lse[...] = top + jnp.log(total) * LOG2E

    def item_rows(kind, qi, t, hot):
        w = jnp.exp2(sbuf[kind, qi, pl.ds(t * H, H), :] * C2 - lse[pl.ds(qi, 1), :])
        if hot:
            places = lax.broadcasted_iota(jnp.int32, (H, N), 0) + t * H
            w = jnp.where(places == pos_ref[...], w - 1.0, w)
        w = w.astype(BF16)
        gbuf[kind, qi, pl.ds(t * H, H), :] = w
        acc[pl.ds(t * H, H), :] += jnp.dot(w, qbuf[qi], preferred_element_type=F32)

    def items_of(kind, lo, hi, t, fresh=True):
        if fresh:
            acc[pl.ds(t * H, H), :] = jnp.zeros((H, D), F32)

        def one(qi, carry):
            item_rows(kind, qi, t, False)
            return carry

        lax.fori_loop(lo, hi, one, 0)

    for t in range(2):
        rows = pl.ds(t * H, H)
        items_of(1, 0, me, t)
        pk[0, rows, :] = acc[rows, :].astype(BF16)
        sent.append(send(18 + t, half(pk, 0, t), half(pr, 0, t), xm))
    for t in range(2):
        items_of(0, 0, 8, t)
    for t in range(2):
        rows = pl.ds(t * H, H)
        arrived(18 + t, half(pr, 0, t))
        pk[1, rows, :] = (acc[rows, :] + pr[0, rows, :].astype(F32)).astype(BF16)
        sent.append(send(20 + t, half(pk, 1, t), half(pr, 1, t), xm))
    for t in range(2):
        items_of(1, me + 1, 8, t)
        item_rows(1, me, t, True)

    def query_part(qi):
        ks = mixed_k(qi)
        part = jnp.dot(kt[1], gbuf[0, qi], preferred_element_type=F32)
        return part + jnp.dot(kt[ks], gbuf[1, qi], preferred_element_type=F32)

    def give(o, carry):
        p = (me + o) % 8
        dqs[o] = query_part(p).astype(BF16)
        pltpu.make_async_remote_copy(
            src_ref=dqs.at[o], dst_ref=dqr.at[o], send_sem=dq_s.at[o], recv_sem=dq_r.at[o],
            device_id=group(p), device_id_type=MESH,
        ).start()
        return carry

    lax.fori_loop(1, 8, give, 0)

    for t in range(2):
        rows = pl.ds(t * H, H)
        arrived(20 + t, half(pr, 1, t))
        dk_ref[rows, :] = (SCALE * (acc[rows, :] + pr[1, rows, :].astype(F32))).astype(BF16)

    total = query_part(me)
    for o in range(1, 8):
        pltpu.make_async_remote_copy(
            src_ref=dqs.at[o], dst_ref=dqr.at[o], send_sem=dq_s.at[o], recv_sem=dq_r.at[o],
            device_id=xp, device_id_type=MESH,
        ).wait()
        total = total + dqr[o].astype(F32)
    dq_ref[...] = (SCALE * total).T.astype(BF16)

    for copy in sent:
        copy.wait_send()
    for copy in stats:
        copy.wait_send()


def main_call(queries, items, positives):
    vmem = pl.BlockSpec(memory_space=pltpu.VMEM)
    hbm = pl.BlockSpec(memory_space=pl.ANY)
    dma = pltpu.SemaphoreType.DMA
    return pl.pallas_call(
        main_kernel,
        out_shape=(jax.ShapeDtypeStruct((N, D), BF16), jax.ShapeDtypeStruct((N, D), BF16)),
        in_specs=[hbm, hbm, vmem],
        out_specs=(vmem, vmem),
        scratch_shapes=[
            pltpu.VMEM((8, N, D), BF16),
            pltpu.VMEM((3, N, D), BF16),
            pltpu.VMEM((2, 8, N, N), F32),
            pltpu.VMEM((2, 8, N, N), BF16),
            pltpu.VMEM((3, D, N), BF16),
            pltpu.VMEM((2, 8, N), F32),
            pltpu.VMEM((8, 8, N), F32),
            pltpu.VMEM((8, N), F32),
            pltpu.VMEM((N, D), F32),
            pltpu.VMEM((2, N, D), BF16),
            pltpu.VMEM((2, N, D), BF16),
            pltpu.VMEM((8, D, N), BF16),
            pltpu.VMEM((8, D, N), BF16),
            dma((2,)), dma((22,)), dma((22,)), dma((7,)), dma((7,)), dma((8,)), dma((8,)),
        ],
        compiler_params=pltpu.CompilerParams(
            collective_id=0, has_side_effects=True, vmem_limit_bytes=60 * 1024 * 1024
        ),
        name="band",
    )(queries, items, positives.reshape(1, N))


def local(queries, items, positives, item_owner, item_row):
    size_rows, feature_width = queries.shape
    devices = lax.axis_size("blk") * lax.axis_size("table")
    capacity = 3 * size_rows // devices
    places = jnp.arange(size_rows, dtype=jnp.int32)
    query_grad, item_grad = main_call(queries, items, positives)
    owners = item_owner[:, 0]
    owner_hot = (owners[:, None] == jnp.arange(devices, dtype=jnp.int32)[None, :]).astype(F32)
    earlier = (places[:, None] > places[None, :]).astype(F32)
    before = jnp.dot(earlier, owner_hot, precision=lax.Precision.HIGHEST)
    ranks = jnp.sum(before * owner_hot, axis=1).astype(jnp.int32)
    slots = owners * capacity + ranks
    send_rows = jnp.zeros((devices * capacity, feature_width), BF16).at[slots].set(item_grad)
    send_ids = jnp.full((devices * capacity,), ROWS_DEV, jnp.int32).at[slots].set(item_row)
    got_rows, got_ids = (
        lax.all_to_all(send_rows, ("blk", "table"), split_axis=0, concat_axis=0, tiled=True),
        lax.all_to_all(send_ids, ("blk", "table"), split_axis=0, concat_axis=0, tiled=True),
    )
    table_grad = (
        jnp.zeros((ROWS_DEV, feature_width), F32)
        .at[got_ids]
        .add(got_rows.astype(F32), mode="drop")
        .astype(BF16)
    )
    return (query_grad, item_grad, table_grad)


def solution(mesh):
    in_specs = (
        P(("blk", "table"), None),
        P(("blk", "table"), None),
        P(("blk", "table")),
        P(("blk", "table"), None),
        P(("blk", "table")),
    )
    out_specs = (P(("blk", "table"), None), P(("blk", "table"), None), P(("blk", "table"), None))
    return jax.shard_map(local, mesh=mesh, in_specs=in_specs, out_specs=out_specs, check_vma=False)
```

```python
import math

import jax
import jax.numpy as jnp
from jax import lax
from jax.experimental import pallas as pl
from jax.experimental.pallas import tpu as pltpu
from jax.sharding import PartitionSpec as P

ROWS_DEV = 16384
N = 512
D = 256
H = 256
DEVS = 128
TABLE = 4
CAP = 12
SCALE = 3.0 / math.sqrt(D)
LOG2E = 1.4426950408889634
C2 = SCALE * LOG2E
MESH = pl.DeviceIdType.MESH
NT = (((1,), (1,)), ((), ()))
NN = (((1,), (0,)), ((), ()))
F32 = jnp.float32
BF16 = jnp.bfloat16


def main_kernel(
    q_hbm, k_hbm, pos_ref, owner_ref, row_ref,
    dq_ref, dk_ref, got_ref, meta_ref,
    qbuf, kbuf, sbuf, gbuf, kt, lk, lst, lse, acc, pk, pr, dqs, dqr,
    keys, ids, got_ids, rows_out,
    lsem, ssem, rsem, st_s, st_r, dq_s, dq_r, ex_s, ex_r,
):
    b = lax.axis_index("blk")
    x = b // 8
    me = b % 8
    z = me // 4
    y = me % 4
    dev = b * TABLE + lax.axis_index("table")

    def slot(r, s):
        return 4 * ((z + s) % 2) + (y + r) % 4

    def group(p):
        return {"blk": x * 8 + p}

    xp = {"blk": ((x + 1) % 4) * 8 + me}
    xm = {"blk": ((x + 3) % 4) * 8 + me}
    yp = group(slot(1, 0))
    ym = group(slot(3, 0))
    zp = group(slot(0, 1))

    own_q = pltpu.make_async_copy(q_hbm, qbuf.at[me], lsem.at[0])
    own_k = pltpu.make_async_copy(k_hbm, kbuf.at[0], lsem.at[1])
    own_q.start()
    own_k.start()

    barrier = pltpu.get_barrier_semaphore()

    def device(p):
        return {"blk": p // TABLE, "table": p % TABLE}

    def greet(o, carry):
        pl.semaphore_signal(barrier, inc=1, device_id=device((dev + o) % DEVS), device_id_type=MESH)
        return carry

    lax.fori_loop(1, DEVS, greet, 0)
    pl.semaphore_wait(barrier, DEVS - 1)
    own_k.wait()
    own_q.wait()

    def half(ref, i, c):
        return ref.at[i, pl.ds(c * H, H)]

    def send(n, src, dst, to):
        copy = pltpu.make_async_remote_copy(
            src_ref=src, dst_ref=dst, send_sem=ssem.at[n], recv_sem=rsem.at[n],
            device_id=to, device_id_type=MESH,
        )
        copy.start()
        return copy

    def arrived(n, ref):
        pltpu.make_async_remote_copy(
            src_ref=ref, dst_ref=ref, send_sem=ssem.at[n], recv_sem=rsem.at[n],
            device_id=xp, device_id_type=MESH,
        ).wait_recv()

    sent = []

    def k_send(n, i, j, c):
        sent.append(send(n, half(kbuf, i, c), half(kbuf, j, c), xp))

    def q_send(n, i, c, to):
        sent.append(send(n, half(qbuf, i, c), half(qbuf, i, c), to))

    k_send(0, 0, 1, 0)
    q_send(4, me, 0, yp)
    q_send(7, me, 1, ym)
    q_send(8, me, 0, zp)
    k_send(1, 0, 1, 1)
    q_send(5, me, 1, yp)
    q_send(6, me, 0, ym)
    q_send(9, me, 1, zp)

    def scores(qi, kind, ks):
        q = qbuf[qi]

        def tile(t, top):
            s = lax.dot_general(kbuf[ks, pl.ds(t * H, H), :], q, NT, preferred_element_type=F32)
            sbuf[kind, qi, pl.ds(t * H, H), :] = s
            return jnp.maximum(top, jnp.max(s.reshape(H // 8, 8, N), axis=0))

        top = lax.fori_loop(0, 2, tile, jnp.full((8, N), -jnp.inf, F32))
        top = jnp.max(top, axis=0, keepdims=True) * C2

        def tile2(t, total):
            s = sbuf[kind, qi, pl.ds(t * H, H), :]
            return total + jnp.sum(jnp.exp2(s * C2 - top).reshape(H // 8, 8, N), axis=0)

        total = lax.fori_loop(0, 2, tile2, jnp.zeros((8, N), F32))
        total = jnp.sum(total, axis=0, keepdims=True)
        lk[kind, pl.ds(qi, 1), :] = top + jnp.log(total) * LOG2E

    def mixed_k(qi):
        return jnp.where(qi >= me, 0, 2)

    scores(me, 1, 0)

    s3, s1, s2, s0 = slot(3, 0), slot(1, 0), slot(2, 0), slot(0, 1)
    t3, t1, t2 = slot(3, 1), slot(1, 1), slot(2, 1)
    arrived(0, half(kbuf, 1, 0))
    k_send(2, 1, 2, 0)
    arrived(4, half(qbuf, s3, 0))
    q_send(10, s3, 0, yp)
    arrived(7, half(qbuf, s1, 1))
    q_send(11, s1, 1, ym)
    arrived(8, half(qbuf, s0, 0))
    q_send(12, s0, 0, yp)
    q_send(14, s0, 0, ym)
    arrived(1, half(kbuf, 1, 1))
    k_send(3, 1, 2, 1)
    arrived(9, half(qbuf, s0, 1))
    q_send(13, s0, 1, yp)
    q_send(15, s0, 1, ym)
    arrived(5, half(qbuf, s3, 1))
    arrived(6, half(qbuf, s1, 0))
    scores(me, 0, 1)
    arrived(10, half(qbuf, s2, 0))
    q_send(16, s2, 0, zp)
    arrived(11, half(qbuf, s2, 1))
    q_send(17, s2, 1, zp)

    owner = owner_ref[...]
    owner_f = owner.astype(F32)
    owner_col = jnp.broadcast_to(owner_f, (8, N)).T[:, 0:1]
    before = lax.broadcasted_iota(jnp.int32, (N, N), 0) < lax.broadcasted_iota(jnp.int32, (N, N), 1)
    rank = jnp.sum(jnp.where((owner_col == owner_f) & before, 1.0, 0.0), axis=0, keepdims=True)
    rank = rank.astype(jnp.int32)
    keys[...] = owner * (2 * CAP) + rank
    row = row_ref[...] + 1
    sub = lax.broadcasted_iota(jnp.int32, (DEVS, N), 0)
    mine = sub == owner
    high = jnp.where(mine, (row // 128).astype(F32), 0.0).astype(BF16)
    low = jnp.where(mine, (row % 128).astype(F32), 0.0).astype(BF16)
    place = jnp.where(sub == rank, 1.0, 0.0).astype(BF16)
    message = 128.0 * lax.dot_general(high, place, NT, preferred_element_type=F32)
    message = message + lax.dot_general(low, place, NT, preferred_element_type=F32)
    ids[...] = message.astype(jnp.int32).reshape(DEVS, 1, 128)
    got_ids[dev] = ids[dev]

    def tell(o, carry):
        p = (dev + o) % DEVS
        pltpu.make_async_remote_copy(
            src_ref=ids.at[p], dst_ref=got_ids.at[dev], send_sem=ex_s.at[0], recv_sem=ex_r.at[0],
            device_id=device(p), device_id_type=MESH,
        ).start()
        return carry

    lax.fori_loop(1, DEVS, tell, 0)

    def first_full(j, carry):
        scores(slot(j, (4 - j) // 4), 0, 1)
        return carry

    lax.fori_loop(0, 4, first_full, 0)
    arrived(2, half(kbuf, 2, 0))
    arrived(3, half(kbuf, 2, 1))

    def turn(i, carry):
        kt[i] = kbuf[i].T
        return carry

    lax.fori_loop(0, 3, turn, 0)

    def first_mixed(j, carry):
        qi = slot(j, (4 - j) // 4)
        scores(qi, 1, mixed_k(qi))
        return carry

    lax.fori_loop(0, 4, first_mixed, 0)
    arrived(12, half(qbuf, t3, 0))
    arrived(14, half(qbuf, t1, 0))
    arrived(13, half(qbuf, t3, 1))
    arrived(15, half(qbuf, t1, 1))
    arrived(16, half(qbuf, t2, 0))
    arrived(17, half(qbuf, t2, 1))

    def last_pairs(j, carry):
        qi = slot(j, 1)
        scores(qi, 0, 1)
        scores(qi, 1, mixed_k(qi))
        return carry

    lax.fori_loop(1, 4, last_pairs, 0)

    a, c = lk[0], lk[1]
    top = jnp.maximum(a, c)
    lst[me] = top + jnp.log(jnp.exp2(a - top) + jnp.exp2(c - top)) * LOG2E
    stats = []
    for o in range(1, 8):
        copy = pltpu.make_async_remote_copy(
            src_ref=lst.at[me], dst_ref=lst.at[me], send_sem=st_s.at[o - 1], recv_sem=st_r.at[o - 1],
            device_id=group((me + o) % 8), device_id_type=MESH,
        )
        copy.start()
        stats.append(copy)
    most = pl.ds(0, DEVS - 1)
    tells = pltpu.make_async_remote_copy(
        src_ref=ids.at[most], dst_ref=got_ids.at[most], send_sem=ex_s.at[0], recv_sem=ex_r.at[0],
        device_id=xp, device_id_type=MESH,
    )
    tells.wait()
    got = got_ids[...].reshape(DEVS, 128)
    count = jnp.sum(jnp.where(got > 0, 1.0, 0.0), axis=1, keepdims=True)
    lane = lax.broadcasted_iota(jnp.int32, (DEVS, DEVS), 1)
    subl = lax.broadcasted_iota(jnp.int32, (DEVS, DEVS), 0)
    below = jnp.where(lane < subl, 1.0, 0.0).astype(BF16)
    counts = jnp.broadcast_to(count, (DEVS, 128)).astype(BF16)
    start = jnp.dot(below, counts, preferred_element_type=F32)[:, 0:1].astype(jnp.int32)
    total_got = jnp.sum(count, axis=0, keepdims=True).astype(jnp.int32)
    source = lax.broadcasted_iota(jnp.int32, (DEVS, 1), 0)

    def listed(t, carry):
        at = lax.broadcasted_iota(jnp.int32, (DEVS, 128), 1) + t * 128
        found = jnp.zeros((8, 128), jnp.int32)
        for c in range(CAP):
            one = got[:, c : c + 1]
            value = (one - 1) + ROWS_DEV * (source * 16 + c)
            hit = jnp.where((at == start + c) & (one > 0), value, 0)
            found = found + jnp.sum(hit.reshape(DEVS // 8, 8, 128), axis=0)
        meta_ref[pl.ds(t, 1), :] = jnp.sum(found, axis=0, keepdims=True)
        return carry

    lax.fori_loop(0, CAP, listed, 0)
    meta_ref[pl.ds(CAP, 1), :] = jnp.broadcast_to(total_got, (1, 128))

    for o in range(1, 8):
        p = (me + 8 - o) % 8
        pltpu.make_async_remote_copy(
            src_ref=lst.at[p], dst_ref=lst.at[p], send_sem=st_s.at[o - 1], recv_sem=st_r.at[o - 1],
            device_id=xp, device_id_type=MESH,
        ).wait_recv()
    top = lst[0]
    for i in range(1, 8):
        top = jnp.maximum(top, lst[i])
    total = jnp.exp2(lst[0] - top)
    for i in range(1, 8):
        total = total + jnp.exp2(lst[i] - top)
    lse[...] = top + jnp.log(total) * LOG2E

    def item_rows(kind, qi, t, hot):
        w = jnp.exp2(sbuf[kind, qi, pl.ds(t * H, H), :] * C2 - lse[pl.ds(qi, 1), :])
        if hot:
            places = lax.broadcasted_iota(jnp.int32, (H, N), 0) + t * H
            w = jnp.where(places == pos_ref[...], w - 1.0, w)
        w = w.astype(BF16)
        gbuf[kind, qi, pl.ds(t * H, H), :] = w
        acc[pl.ds(t * H, H), :] += jnp.dot(w, qbuf[qi], preferred_element_type=F32)

    def items_of(kind, lo, hi, t, fresh=True):
        if fresh:
            acc[pl.ds(t * H, H), :] = jnp.zeros((H, D), F32)

        def one(qi, carry):
            item_rows(kind, qi, t, False)
            return carry

        lax.fori_loop(lo, hi, one, 0)

    for t in range(2):
        rows = pl.ds(t * H, H)
        items_of(1, 0, me, t)
        pk[0, rows, :] = acc[rows, :].astype(BF16)
        sent.append(send(18 + t, half(pk, 0, t), half(pr, 0, t), xm))
    for t in range(2):
        items_of(0, 0, 8, t)
    for t in range(2):
        rows = pl.ds(t * H, H)
        arrived(18 + t, half(pr, 0, t))
        pk[1, rows, :] = (acc[rows, :] + pr[0, rows, :].astype(F32)).astype(BF16)
        sent.append(send(20 + t, half(pk, 1, t), half(pr, 1, t), xm))
    for t in range(2):
        items_of(1, me + 1, 8, t)
        item_rows(1, me, t, True)

    def query_part(qi):
        ks = mixed_k(qi)
        part = jnp.dot(kt[1], gbuf[0, qi], preferred_element_type=F32)
        return part + jnp.dot(kt[ks], gbuf[1, qi], preferred_element_type=F32)

    def give(o, carry):
        p = (me + o) % 8
        dqs[o] = query_part(p).astype(BF16)
        pltpu.make_async_remote_copy(
            src_ref=dqs.at[o], dst_ref=dqr.at[o], send_sem=dq_s.at[o], recv_sem=dq_r.at[o],
            device_id=group(p), device_id_type=MESH,
        ).start()
        return carry

    lax.fori_loop(1, 8, give, 0)

    for t in range(2):
        rows = pl.ds(t * H, H)
        arrived(20 + t, half(pr, 1, t))
        dk_ref[rows, :] = (SCALE * (acc[rows, :] + pr[1, rows, :].astype(F32))).astype(BF16)

    own = pltpu.make_async_copy(rows_out.at[dev], got_ref.at[dev], lsem.at[2])

    def dispatch(g, carry):
        first = ((g + b // 4) % 8) * 16
        at = lax.broadcasted_iota(jnp.int32, (16 * 2 * CAP, N), 0) + first * (2 * CAP)
        left = jnp.where(at == keys[...], 1.0, 0.0).astype(BF16)
        right = jnp.where(at == keys[...] + CAP, 1.0, 0.0).astype(BF16)
        picked = jnp.dot(left, dk_ref[:, 0:128], preferred_element_type=F32)
        picked = picked + jnp.dot(right, dk_ref[:, 128:256], preferred_element_type=F32)
        rows_out[pl.ds(first, 16)] = picked.astype(BF16).reshape(16, 2 * CAP, 128)

        def post(j, carry):
            p = first + j

            @pl.when(p != dev)
            def _():
                pltpu.make_async_remote_copy(
                    src_ref=rows_out.at[p], dst_ref=got_ref.at[dev], send_sem=ex_s.at[1],
                    recv_sem=ex_r.at[1], device_id=device(p), device_id_type=MESH,
                ).start()

            return carry

        lax.fori_loop(0, 16, post, 0)
        return carry

    lax.fori_loop(0, 8, dispatch, 0)
    own.start()

    total = query_part(me)
    for o in range(1, 8):
        pltpu.make_async_remote_copy(
            src_ref=dqs.at[o], dst_ref=dqr.at[o], send_sem=dq_s.at[o], recv_sem=dq_r.at[o],
            device_id=xp, device_id_type=MESH,
        ).wait()
        total = total + dqr[o].astype(F32)
    dq_ref[...] = (SCALE * total).T.astype(BF16)

    own.wait()
    pltpu.make_async_remote_copy(
        src_ref=rows_out.at[most], dst_ref=got_ref.at[most], send_sem=ex_s.at[1],
        recv_sem=ex_r.at[1], device_id=xp, device_id_type=MESH,
    ).wait()
    for copy in sent:
        copy.wait_send()
    for copy in stats:
        copy.wait_send()


def main_call(queries, items, positives, owner, row):
    vmem = pl.BlockSpec(memory_space=pltpu.VMEM)
    hbm = pl.BlockSpec(memory_space=pl.ANY)
    dma = pltpu.SemaphoreType.DMA
    return pl.pallas_call(
        main_kernel,
        out_shape=(
            jax.ShapeDtypeStruct((N, D), BF16),
            jax.ShapeDtypeStruct((N, D), BF16),
            jax.ShapeDtypeStruct((DEVS, 2 * CAP, 128), BF16),
            jax.ShapeDtypeStruct((CAP + 1, 128), jnp.int32),
        ),
        in_specs=[hbm, hbm, vmem, vmem, vmem],
        out_specs=(vmem, vmem, hbm, vmem),
        scratch_shapes=[
            pltpu.VMEM((8, N, D), BF16),
            pltpu.VMEM((3, N, D), BF16),
            pltpu.VMEM((2, 8, N, N), F32),
            pltpu.VMEM((2, 8, N, N), BF16),
            pltpu.VMEM((3, D, N), BF16),
            pltpu.VMEM((2, 8, N), F32),
            pltpu.VMEM((8, 8, N), F32),
            pltpu.VMEM((8, N), F32),
            pltpu.VMEM((N, D), F32),
            pltpu.VMEM((2, N, D), BF16),
            pltpu.VMEM((2, N, D), BF16),
            pltpu.VMEM((8, D, N), BF16),
            pltpu.VMEM((8, D, N), BF16),
            pltpu.VMEM((1, N), jnp.int32),
            pltpu.VMEM((DEVS, 1, 128), jnp.int32),
            pltpu.VMEM((DEVS, 1, 128), jnp.int32),
            pltpu.VMEM((DEVS, 2 * CAP, 128), BF16),
            dma((3,)), dma((22,)), dma((22,)), dma((7,)), dma((7,)), dma((8,)), dma((8,)),
            dma((2,)), dma((2,)),
        ],
        compiler_params=pltpu.CompilerParams(
            collective_id=0, has_side_effects=True, vmem_limit_bytes=60 * 1024 * 1024
        ),
        name="band",
    )(queries, items, positives.reshape(1, N), owner.reshape(1, N), row.reshape(1, N))


PIECE = 1024


def table_kernel(meta, got, out, tab, rows, stage, sem):
    def clear(i, carry):
        tab[:, pl.ds(pl.multiple_of(i * 128, 128), 128), :] = jnp.zeros((2, 128, 128), F32)
        return carry

    lax.fori_loop(0, ROWS_DEV // 128, clear, 0)

    def widen(i, carry):
        rows[pl.ds(i * 16, 16)] = got[pl.ds(i * 16, 16)].astype(F32)
        return carry

    lax.fori_loop(0, DEVS // 16, widen, 0)

    def add(n, carry):
        value = meta[n // 128, n % 128]
        to = value % ROWS_DEV
        place = value // ROWS_DEV
        source, c = place // 16, place % 16
        tab[0, pl.ds(to, 1), :] += rows[source, pl.ds(c, 1), :]
        tab[1, pl.ds(to, 1), :] += rows[source, pl.ds(c + CAP, 1), :]
        return carry

    lax.fori_loop(0, meta[CAP, 0], add, 0)

    def piece(i):
        at = i * PIECE if isinstance(i, int) else pl.multiple_of(i * PIECE, PIECE)
        return pltpu.make_async_copy(stage.at[i % 2], out.at[pl.ds(at, PIECE)], sem.at[i % 2])

    def store(i, carry):
        @pl.when(i >= 2)
        def _():
            piece(i - 2).wait()

        def turn(j, carry):
            at = pl.multiple_of(i * PIECE + j * 128, 128)
            to = pl.ds(pl.multiple_of(j * 128, 128), 128)
            stage[i % 2, to, 0:128] = tab[0, pl.ds(at, 128), :].astype(BF16)
            stage[i % 2, to, 128:256] = tab[1, pl.ds(at, 128), :].astype(BF16)
            return carry

        lax.fori_loop(0, PIECE // 128, turn, 0)
        piece(i).start()
        return carry

    pieces = ROWS_DEV // PIECE
    lax.fori_loop(0, pieces, store, 0)
    piece(pieces - 2).wait()
    piece(pieces - 1).wait()


def table_call(meta, got):
    return pl.pallas_call(
        table_kernel,
        out_shape=jax.ShapeDtypeStruct((ROWS_DEV, D), BF16),
        in_specs=[pl.BlockSpec(memory_space=pltpu.SMEM), pl.BlockSpec(memory_space=pltpu.VMEM)],
        out_specs=pl.BlockSpec(memory_space=pl.ANY),
        scratch_shapes=[
            pltpu.VMEM((2, ROWS_DEV, 128), F32),
            pltpu.VMEM((DEVS, 2 * CAP, 128), F32),
            pltpu.VMEM((2, PIECE, D), BF16),
            pltpu.SemaphoreType.DMA((2,)),
        ],
        compiler_params=pltpu.CompilerParams(vmem_limit_bytes=60 * 1024 * 1024),
        name="table",
    )(meta, got)


def local(queries, items, positives, item_owner, item_row):
    query_grad, item_grad, got, meta = main_call(queries, items, positives, item_owner, item_row)
    return (query_grad, item_grad, table_call(meta, got))


def solution(mesh):
    in_specs = (
        P(("blk", "table"), None),
        P(("blk", "table"), None),
        P(("blk", "table")),
        P(("blk", "table"), None),
        P(("blk", "table")),
    )
    out_specs = (P(("blk", "table"), None), P(("blk", "table"), None), P(("blk", "table"), None))
    return jax.shard_map(local, mesh=mesh, in_specs=in_specs, out_specs=out_specs, check_vma=False)
```

```python
import math

import jax
import jax.numpy as jnp
from jax import lax
from jax.experimental import pallas as pl
from jax.experimental.pallas import tpu as pltpu
from jax.sharding import PartitionSpec as P

ROWS_DEV = 16384
N = 512
D = 256
H = 256
DEVS = 128
TABLE = 4
CAP = 12
BLK = 32
LIST = 13
SCALE = 3.0 / math.sqrt(D)
LOG2E = 1.4426950408889634
C2 = SCALE * LOG2E
MESH = pl.DeviceIdType.MESH
NT = (((1,), (1,)), ((), ()))
F32 = jnp.float32
BF16 = jnp.bfloat16


def listing(got, meta_ref, posb, valb):
    lane = lax.broadcasted_iota(jnp.int32, (DEVS, 128), 1)
    subl = lax.broadcasted_iota(jnp.int32, (DEVS, 128), 0)
    ident = got.astype(F32)
    turned = ident.T
    number = turned.astype(jnp.int32) - 1
    high = lax.shift_right_arithmetic(number, 7)
    low = lax.bitwise_and(number, 127)

    def hot(which, c):
        return jnp.where(subl == which[c : c + 1, :], 1.0, 0.0)

    counts = jnp.zeros((DEVS, 128), F32)
    for c in range(CAP):
        counts = counts + lax.dot_general(
            hot(low, c).astype(BF16), hot(high, c).astype(BF16), NT, preferred_element_type=F32
        )
    counts = counts.astype(BF16)
    named = jnp.zeros((DEVS, 128), F32)
    for c in range(CAP):
        by_low = jnp.dot(counts, hot(high, c).astype(BF16), preferred_element_type=F32)
        times = jnp.sum(by_low * hot(low, c), axis=0, keepdims=True)
        named = jnp.where(subl == c, times, named)
    named = named.T
    first = jnp.where(named == 1.0, 1.0, 0.0).astype(BF16)
    again = jnp.where(named > 1.0, 1.0, 0.0).astype(BF16)
    upper = jnp.where(subl < lane, 1.0, 0.0).astype(BF16)
    lower = jnp.where(lane < subl, 1.0, 0.0).astype(BF16)
    ones = jnp.ones((DEVS, 128), BF16)

    def ranked(flags):
        per_row = jnp.dot(flags, ones, preferred_element_type=F32)
        place = jnp.dot(lower, per_row.astype(BF16), preferred_element_type=F32)
        place = place + jnp.dot(flags, upper, preferred_element_type=F32)
        return place.astype(jnp.int32), jnp.sum(per_row, axis=0, keepdims=True).astype(jnp.int32)

    first_at, first_count = ranked(first)
    again_at, again_count = ranked(again)
    pos = jnp.where(first > 0, first_at, jnp.where(again > 0, LIST * 128 - 1 - again_at, -1))
    value = got + 32768 * (subl * (2 * CAP) + lane)
    for c in range(CAP):
        posb[c] = jnp.broadcast_to(pos[:, c : c + 1], (DEVS, 128))
        valb[c] = jnp.broadcast_to(value[:, c : c + 1], (DEVS, 128))

    def listed(t, carry):
        at = lane + t * 128
        found = jnp.zeros((8, 128), jnp.int32)
        for c in range(CAP):
            hit = jnp.where(posb[c] == at, valb[c], 0)
            found = found + jnp.sum(hit.reshape(DEVS // 8, 8, 128), axis=0)
        found = jnp.sum(found, axis=0, keepdims=True)
        meta_ref[pl.ds(t, 1), :] = jnp.where(found > 0, found - 1, ROWS_DEV)
        return carry

    lax.fori_loop(0, LIST, listed, 0)
    one = lax.broadcasted_iota(jnp.int32, (1, 128), 1)
    meta_ref[pl.ds(LIST, 1), :] = jnp.where(one == 0, first_count, again_count)


def main_kernel(
    q_hbm, k_hbm, pos_ref, owner_ref, row_ref,
    dq_ref, dk_ref, got_ref, meta_ref,
    qbuf, kbuf, sbuf, gbuf, kt, lk, lst, lse, acc, pk, pr, tx, rx, keep,
    keys, ids, got_ids, rows_out, posb, valb,
    lsem, ssem, rsem, st_s, st_r, dq_s, dq_r, ex_s, ex_r, token,
):
    b = lax.axis_index("blk")
    tab = lax.axis_index("table")
    x = lax.div(b, 8)
    me = lax.rem(b, 8)
    z = lax.div(me, 4)
    y = lax.rem(me, 4)
    dev = b * TABLE + tab

    def slot(r, s):
        return 4 * lax.rem(z + s, 2) + lax.rem(y + r, 4)

    def group(p):
        return {"blk": x * 8 + p}

    def along(o):
        return {"blk": lax.rem(x + o, 4) * 8 + me}

    def sibling(o):
        return {"table": lax.rem(tab + o, TABLE)}

    xp, xm = along(1), along(3)
    yp = group(slot(1, 0))
    ym = group(slot(3, 0))
    zp = group(slot(0, 1))

    own_q = pltpu.make_async_copy(q_hbm, qbuf.at[me], lsem.at[0])
    own_k = pltpu.make_async_copy(k_hbm, kbuf.at[0], lsem.at[1])
    own_q.start()
    own_k.start()

    barrier = pltpu.get_barrier_semaphore()
    peers = [group(lax.rem(me + o, 8)) for o in range(1, 8)]
    tables = [sibling(o) for o in range(1, TABLE)]
    for to in peers + [along(o) for o in range(1, 4)] + tables:
        pl.semaphore_signal(barrier, inc=1, device_id=to, device_id_type=MESH)
    pl.semaphore_wait(barrier, 13)
    own_k.wait()
    own_q.wait()

    def half(ref, i, c):
        return ref.at[i, pl.ds(c * H, H)]

    def send(n, src, dst, to):
        copy = pltpu.make_async_remote_copy(
            src_ref=src, dst_ref=dst, send_sem=ssem.at[n], recv_sem=rsem.at[n],
            device_id=to, device_id_type=MESH,
        )
        copy.start()
        return copy

    def arrived(n, ref):
        pltpu.make_async_remote_copy(
            src_ref=ref, dst_ref=ref, send_sem=ssem.at[n], recv_sem=rsem.at[n],
            device_id=xp, device_id_type=MESH,
        ).wait_recv()

    sent = []

    def k_send(n, i, j, c):
        sent.append(send(n, half(kbuf, i, c), half(kbuf, j, c), xp))

    def q_send(n, i, c, to):
        sent.append(send(n, half(qbuf, i, c), half(qbuf, i, c), to))

    k_send(0, 0, 1, 0)
    q_send(4, me, 0, yp)
    q_send(7, me, 1, ym)
    q_send(8, me, 0, zp)
    k_send(1, 0, 1, 1)
    q_send(5, me, 1, yp)
    q_send(6, me, 0, ym)
    q_send(9, me, 1, zp)

    def scores(qi, kind, ks):
        q = qbuf[qi]

        def tile(t, top):
            s = lax.dot_general(kbuf[ks, pl.ds(t * H, H), :], q, NT, preferred_element_type=F32)
            sbuf[kind, qi, pl.ds(t * H, H), :] = s
            return jnp.maximum(top, jnp.max(s.reshape(H // 8, 8, N), axis=0))

        top = lax.fori_loop(0, 2, tile, jnp.full((8, N), -jnp.inf, F32))
        top = jnp.max(top, axis=0, keepdims=True) * C2

        def tile2(t, total):
            s = sbuf[kind, qi, pl.ds(t * H, H), :]
            return total + jnp.sum(jnp.exp2(s * C2 - top).reshape(H // 8, 8, N), axis=0)

        total = lax.fori_loop(0, 2, tile2, jnp.zeros((8, N), F32))
        total = jnp.sum(total, axis=0, keepdims=True)
        lk[kind, pl.ds(qi, 1), :] = top + jnp.log(total) * LOG2E

    def mixed_k(qi):
        return jnp.where(qi >= me, 0, 2)

    scores(me, 1, 0)

    s3, s1, s2, s0 = slot(3, 0), slot(1, 0), slot(2, 0), slot(0, 1)
    t3, t1, t2 = slot(3, 1), slot(1, 1), slot(2, 1)
    arrived(0, half(kbuf, 1, 0))
    k_send(2, 1, 2, 0)
    arrived(4, half(qbuf, s3, 0))
    q_send(10, s3, 0, yp)
    arrived(7, half(qbuf, s1, 1))
    q_send(11, s1, 1, ym)
    arrived(8, half(qbuf, s0, 0))
    q_send(12, s0, 0, yp)
    q_send(14, s0, 0, ym)
    arrived(1, half(kbuf, 1, 1))
    k_send(3, 1, 2, 1)
    arrived(9, half(qbuf, s0, 1))
    q_send(13, s0, 1, yp)
    q_send(15, s0, 1, ym)
    arrived(5, half(qbuf, s3, 1))
    arrived(6, half(qbuf, s1, 0))
    scores(me, 0, 1)
    arrived(10, half(qbuf, s2, 0))
    q_send(16, s2, 0, zp)
    arrived(11, half(qbuf, s2, 1))
    q_send(17, s2, 1, zp)

    owner = owner_ref[...]
    owner_f = owner.astype(F32)
    owner_col = jnp.broadcast_to(owner_f, (8, N)).T[:, 0:1]
    before = lax.broadcasted_iota(jnp.int32, (N, N), 0) < lax.broadcasted_iota(jnp.int32, (N, N), 1)
    rank = jnp.sum(jnp.where((owner_col == owner_f) & before, 1.0, 0.0), axis=0, keepdims=True)
    rank = rank.astype(jnp.int32)
    away = owner - b * TABLE
    away = jnp.where(away < 0, away + DEVS, away)
    keys[...] = away * (2 * CAP) + rank
    row = row_ref[...] + 1
    sub = lax.broadcasted_iota(jnp.int32, (DEVS, N), 0)
    mine = sub == away
    high = jnp.where(mine, (row // 128).astype(F32), 0.0).astype(BF16)
    low = jnp.where(mine, (row % 128).astype(F32), 0.0).astype(BF16)
    place = jnp.where(sub == rank, 1.0, 0.0).astype(BF16)
    message = 128.0 * lax.dot_general(high, place, NT, preferred_element_type=F32)
    message = message + lax.dot_general(low, place, NT, preferred_element_type=F32)
    ids[...] = message.astype(jnp.int32).reshape(DEVS, 1, 128)
    got_ids[dev] = ids[tab]

    for to in tables:
        pl.semaphore_signal(token.at[0], inc=1, device_id=to, device_id_type=MESH)
    pl.semaphore_wait(token.at[0], TABLE - 1)
    for to in peers:
        pl.semaphore_signal(token.at[1], inc=1, device_id=to, device_id_type=MESH)
    pl.semaphore_wait(token.at[1], 7)

    def post(src, dst, n, o, t):
        pltpu.make_async_remote_copy(
            src_ref=src.at[o * TABLE + t], dst_ref=dst.at[dev], send_sem=ex_s.at[n], recv_sem=ex_r.at[n],
            device_id={"blk": lax.rem(b + o, BLK), "table": t}, device_id_type=MESH,
        ).start()

    def post_near(src, dst, n):
        for t in range(TABLE):

            @pl.when(tab != t)
            def _():
                post(src, dst, n, 0, t)

    def tell(o, carry):
        for t in range(TABLE):
            post(ids, got_ids, 0, o, t)
        return carry

    post_near(ids, got_ids, 0)
    lax.fori_loop(1, BLK, tell, 0)

    def first_full(j, carry):
        scores(slot(j, (4 - j) // 4), 0, 1)
        return carry

    lax.fori_loop(0, 4, first_full, 0)
    arrived(2, half(kbuf, 2, 0))
    arrived(3, half(kbuf, 2, 1))

    def turn(i, carry):
        kt[i] = kbuf[i].T
        return carry

    lax.fori_loop(0, 3, turn, 0)

    def first_mixed(j, carry):
        qi = slot(j, (4 - j) // 4)
        scores(qi, 1, mixed_k(qi))
        return carry

    lax.fori_loop(0, 4, first_mixed, 0)
    def last_pairs(r):
        qi = slot(r, 1)
        scores(qi, 0, 1)
        scores(qi, 1, mixed_k(qi))

    arrived(12, half(qbuf, t3, 0))
    arrived(13, half(qbuf, t3, 1))
    last_pairs(3)
    arrived(14, half(qbuf, t1, 0))
    arrived(15, half(qbuf, t1, 1))
    last_pairs(1)
    arrived(16, half(qbuf, t2, 0))
    arrived(17, half(qbuf, t2, 1))
    last_pairs(2)

    a, c = lk[0], lk[1]
    top = jnp.maximum(a, c)
    lst[me] = top + jnp.log(jnp.exp2(a - top) + jnp.exp2(c - top)) * LOG2E
    stats = []
    for o in range(1, 8):
        copy = pltpu.make_async_remote_copy(
            src_ref=lst.at[me], dst_ref=lst.at[me], send_sem=st_s.at[o - 1], recv_sem=st_r.at[o - 1],
            device_id=group(lax.rem(me + o, 8)), device_id_type=MESH,
        )
        copy.start()
        stats.append(copy)
    most = pl.ds(0, DEVS - 1)
    tells = pltpu.make_async_remote_copy(
        src_ref=ids.at[most], dst_ref=got_ids.at[most], send_sem=ex_s.at[0], recv_sem=ex_r.at[0],
        device_id=xp, device_id_type=MESH,
    )
    tells.wait()
    listing(got_ids[...].reshape(DEVS, 128), meta_ref, posb, valb)

    for o in range(1, 8):
        p = lax.rem(me + 8 - o, 8)
        pltpu.make_async_remote_copy(
            src_ref=lst.at[p], dst_ref=lst.at[p], send_sem=st_s.at[o - 1], recv_sem=st_r.at[o - 1],
            device_id=xp, device_id_type=MESH,
        ).wait_recv()
    top = lst[0]
    for i in range(1, 8):
        top = jnp.maximum(top, lst[i])
    total = jnp.exp2(lst[0] - top)
    for i in range(1, 8):
        total = total + jnp.exp2(lst[i] - top)
    lse[...] = top + jnp.log(total) * LOG2E

    def item_rows(kind, qi, t, hot):
        w = jnp.exp2(sbuf[kind, qi, pl.ds(t * H, H), :] * C2 - lse[pl.ds(qi, 1), :])
        if hot:
            places = lax.broadcasted_iota(jnp.int32, (H, N), 0) + t * H
            w = jnp.where(places == pos_ref[...], w - 1.0, w)
        w = w.astype(BF16)
        gbuf[kind, qi, pl.ds(t * H, H), :] = w
        acc[pl.ds(t * H, H), :] += jnp.dot(w, qbuf[qi], preferred_element_type=F32)

    def items_of(kind, lo, hi, t, fresh=True):
        if fresh:
            acc[pl.ds(t * H, H), :] = jnp.zeros((H, D), F32)

        def one(qi, carry):
            item_rows(kind, qi, t, False)
            return carry

        lax.fori_loop(lo, hi, one, 0)

    for t in range(2):
        rows = pl.ds(t * H, H)
        items_of(1, 0, me, t)
        pk[0, rows, :] = acc[rows, :].astype(BF16)
        sent.append(send(18 + t, half(pk, 0, t), half(pr, 0, t), xm))
    for t in range(2):
        items_of(0, 0, 8, t)
    for t in range(2):
        rows = pl.ds(t * H, H)
        arrived(18 + t, half(pr, 0, t))
        pk[1, rows, :] = (acc[rows, :] + pr[0, rows, :].astype(F32)).astype(BF16)
        sent.append(send(20 + t, half(pk, 1, t), half(pr, 1, t), xm))
    for t in range(2):
        items_of(1, me + 1, 8, t)
        item_rows(1, me, t, True)

    def query_part(qi):
        ks = mixed_k(qi)
        part = jnp.dot(kt[1], gbuf[0, qi], preferred_element_type=F32)
        return part + jnp.dot(kt[ks], gbuf[1, qi], preferred_element_type=F32)

    def give(i, h, value, to):
        tx[i, h] = value.astype(BF16)
        copy = pltpu.make_async_remote_copy(
            src_ref=tx.at[i, h], dst_ref=rx.at[i, h], send_sem=dq_s.at[2 * i + h],
            recv_sem=dq_r.at[2 * i + h], device_id=to, device_id_type=MESH,
        )
        copy.start()
        sent.append(copy)

    def given(i, h):
        pltpu.make_async_remote_copy(
            src_ref=rx.at[i, h], dst_ref=rx.at[i, h], send_sem=dq_s.at[2 * i + h],
            recv_sem=dq_r.at[2 * i + h], device_id=xp, device_id_type=MESH,
        ).wait_recv()
        return rx[i, h].astype(F32)

    for i, r, to in ((0, 2, zp), (4, 1, yp), (5, 3, ym)):
        part = query_part(slot(r, 1))
        give(i, 0, part[:, :H], to)
        give(i, 1, part[:, H:], to)
    part = query_part(slot(1, 0))
    give(2, 1, part[:, H:], yp)
    keep[0] = part[:, :H]
    part = query_part(slot(3, 0))
    give(3, 0, part[:, :H], ym)
    keep[1] = part[:, H:]
    part = query_part(slot(0, 1))
    keep[2] = part[:, :H]
    keep[3] = part[:, H:]
    part = query_part(slot(2, 0))
    keep[4] = part[:, :H]
    keep[5] = part[:, H:]
    give(1, 0, keep[4] + given(0, 0), yp)
    give(1, 1, keep[5] + given(0, 1), ym)

    for t in range(2):
        rows = pl.ds(t * H, H)
        arrived(20 + t, half(pr, 1, t))
        dk_ref[rows, :] = (SCALE * (acc[rows, :] + pr[1, rows, :].astype(F32))).astype(BF16)

    own = pltpu.make_async_copy(rows_out.at[tab], got_ref.at[dev], lsem.at[2])

    def dispatch(g, carry):
        at = lax.broadcasted_iota(jnp.int32, (16 * 2 * CAP, N), 0) + g * (16 * 2 * CAP)
        left = jnp.where(at == keys[...], 1.0, 0.0).astype(BF16)
        right = jnp.where(at == keys[...] + CAP, 1.0, 0.0).astype(BF16)
        picked = jnp.dot(left, dk_ref[:, 0:128], preferred_element_type=F32)
        picked = picked + jnp.dot(right, dk_ref[:, 128:256], preferred_element_type=F32)
        rows_out[pl.ds(g * 16, 16)] = picked.astype(BF16).reshape(16, 2 * CAP, 128)

        @pl.when(g == 0)
        def _():
            own.start()
            post_near(rows_out, got_ref, 1)

        def four(j, c):
            for t in range(TABLE):
                post(rows_out, got_ref, 1, g * 4 + j, t)
            return c

        lax.fori_loop(jnp.where(g == 0, 1, 0), 4, four, 0)
        return carry

    lax.fori_loop(0, 8, dispatch, 0)

    for h in range(2):
        give(6, h, keep[2 + h] + given(4, h) + given(5, h), zp)
    give(2, 0, keep[0] + given(1, 0), yp)
    give(3, 1, keep[1] + given(1, 1), ym)
    part = query_part(me)
    for h in range(2):
        mine = part[:, h * H : (h + 1) * H] + given(2, h) + given(3, h) + given(6, h)
        dq_ref[pl.ds(h * H, H), :] = (SCALE * mine).T.astype(BF16)

    own.wait()
    pltpu.make_async_remote_copy(
        src_ref=rows_out.at[most], dst_ref=got_ref.at[most], send_sem=ex_s.at[1],
        recv_sem=ex_r.at[1], device_id=xp, device_id_type=MESH,
    ).wait()
    for copy in sent:
        copy.wait_send()
    for copy in stats:
        copy.wait_send()


def main_call(queries, items, positives, owner, row):
    vmem = pl.BlockSpec(memory_space=pltpu.VMEM)
    hbm = pl.BlockSpec(memory_space=pl.ANY)
    dma = pltpu.SemaphoreType.DMA
    return pl.pallas_call(
        main_kernel,
        out_shape=(
            jax.ShapeDtypeStruct((N, D), BF16),
            jax.ShapeDtypeStruct((N, D), BF16),
            jax.ShapeDtypeStruct((DEVS, 2 * CAP, 128), BF16),
            jax.ShapeDtypeStruct((LIST + 1, 128), jnp.int32),
        ),
        in_specs=[hbm, hbm, vmem, vmem, vmem],
        out_specs=(vmem, vmem, hbm, vmem),
        scratch_shapes=[
            pltpu.VMEM((8, N, D), BF16),
            pltpu.VMEM((3, N, D), BF16),
            pltpu.VMEM((2, 8, N, N), F32),
            pltpu.VMEM((2, 8, N, N), BF16),
            pltpu.VMEM((3, D, N), BF16),
            pltpu.VMEM((2, 8, N), F32),
            pltpu.VMEM((8, 8, N), F32),
            pltpu.VMEM((8, N), F32),
            pltpu.VMEM((N, D), F32),
            pltpu.VMEM((2, N, D), BF16),
            pltpu.VMEM((2, N, D), BF16),
            pltpu.VMEM((7, 2, D, H), BF16),
            pltpu.VMEM((7, 2, D, H), BF16),
            pltpu.VMEM((6, D, H), F32),
            pltpu.VMEM((1, N), jnp.int32),
            pltpu.VMEM((DEVS, 1, 128), jnp.int32),
            pltpu.VMEM((DEVS, 1, 128), jnp.int32),
            pltpu.VMEM((DEVS, 2 * CAP, 128), BF16),
            pltpu.VMEM((CAP, DEVS, 128), jnp.int32),
            pltpu.VMEM((CAP, DEVS, 128), jnp.int32),
            dma((3,)), dma((22,)), dma((22,)), dma((7,)), dma((7,)), dma((14,)), dma((14,)),
            dma((2,)), dma((2,)), pltpu.SemaphoreType.REGULAR((2,)),
        ],
        compiler_params=pltpu.CompilerParams(
            collective_id=0, has_side_effects=True, vmem_limit_bytes=60 * 1024 * 1024
        ),
        name="band",
    )(queries, items, positives.reshape(1, N), owner.reshape(1, N), row.reshape(1, N))


PIECE = 1024
SLOTS = 8
STEP = 8


def table_kernel(meta, got, out, left, right, rows, stage, sem):
  def clear(i, carry):
      to = pl.ds(pl.multiple_of(i * 512, 512), 512)
      left[to, :] = jnp.zeros((512, 128), F32)
      right[to, :] = jnp.zeros((512, 128), F32)
      return carry
  lax.fori_loop(0, ROWS_DEV // 512, clear, 0)
  def widen(i, carry):
      to = pl.ds(pl.multiple_of(i * 384, 384), 384)
      rows[to, :] = got[pl.ds(i * 16, 16)].astype(F32).reshape(384,128)
      return carry
  lax.fori_loop(0, DEVS // 16, widen, 0)
  def entry(n):
      v = meta[lax.shift_right_logical(n, 7), lax.bitwise_and(n, 127)]
      to = lax.bitwise_and(v, 32767); at = lax.shift_right_logical(v, 15)
      return pl.ds(to, 1), rows[pl.ds(at, 1), :], rows[pl.ds(at + CAP, 1), :]
  def place(i, carry):
      for j in range(STEP):
          to, a, b = entry(i * STEP + j)
          left[to, :] = a
          right[to, :] = b
      return carry
  lax.fori_loop(0, lax.div(meta[LIST, 0] + STEP - 1, STEP), place, 0)
  def again(i, carry):
      for j in range(STEP):
          to, a, b = entry(LIST * 128 - 1 - i * STEP - j)
          left[to, :] += a
          right[to, :] += b
      return carry
  lax.fori_loop(0, lax.div(meta[LIST, 1] + STEP - 1, STEP), again, 0)
  def piece(i):
      at = i * PIECE if isinstance(i, int) else pl.multiple_of(i * PIECE, PIECE)
      return pltpu.make_async_copy(stage.at[lax.rem(i, SLOTS)], out.at[pl.ds(at, PIECE)], sem.at[lax.rem(i, SLOTS)])
  def store(i, carry):
      @pl.when(i >= SLOTS)
      def _():
          piece(i - SLOTS).wait()
      s = lax.rem(i, SLOTS)
      def turn(j, carry):
          at = pl.ds(pl.multiple_of(i * PIECE + j * 256, 256), 256)
          to = pl.ds(pl.multiple_of(j * 256, 256), 256)
          stage[s, to, 0:128] = left[at, :].astype(BF16)
          stage[s, to, 128:256] = right[at, :].astype(BF16)
          return carry
      lax.fori_loop(0, PIECE // 256, turn, 0)
      piece(i).start()
      return carry
  pieces = ROWS_DEV // PIECE
  lax.fori_loop(0, pieces, store, 0)
  for k in range(SLOTS): piece(pieces - SLOTS + k).wait()


def table_call(meta, got):
    return pl.pallas_call(
        table_kernel,
        out_shape=jax.ShapeDtypeStruct((ROWS_DEV, D), BF16),
        in_specs=[pl.BlockSpec(memory_space=pltpu.SMEM), pl.BlockSpec(memory_space=pltpu.VMEM)],
        out_specs=pl.BlockSpec(memory_space=pl.ANY),
        scratch_shapes=[
            pltpu.VMEM((ROWS_DEV + 8, 128), F32),
            pltpu.VMEM((ROWS_DEV + 8, 128), F32),
            pltpu.VMEM((DEVS * 2 * CAP, 128), F32),
            pltpu.VMEM((SLOTS, PIECE, D), BF16),
            pltpu.SemaphoreType.DMA((SLOTS,)),
        ],
        compiler_params=pltpu.CompilerParams(vmem_limit_bytes=60 * 1024 * 1024),
        name="table",
    )(meta, got)


def local(queries, items, positives, item_owner, item_row):
    query_grad, item_grad, got, meta = main_call(queries, items, positives, item_owner, item_row)
    return (query_grad, item_grad, table_call(meta, got))


def solution(mesh):
    in_specs = (
        P(("blk", "table"), None),
        P(("blk", "table"), None),
        P(("blk", "table")),
        P(("blk", "table"), None),
        P(("blk", "table")),
    )
    out_specs = (P(("blk", "table"), None), P(("blk", "table"), None), P(("blk", "table"), None))
    return jax.shard_map(local, mesh=mesh, in_specs=in_specs, out_specs=out_specs, check_vma=False)
```

```python
import math

import jax
import jax.numpy as jnp
from jax import lax
from jax.experimental import pallas as pl
from jax.experimental.pallas import tpu as pltpu
from jax.sharding import PartitionSpec as P

ROWS_DEV = 16384
N = 512
D = 256
H = 256
DEVS = 128
TABLE = 4
CAP = 12
BLK = 32
LIST = 13
SCALE = 3.0 / math.sqrt(D)
LOG2E = 1.4426950408889634
C2 = SCALE * LOG2E
MESH = pl.DeviceIdType.MESH
NT = (((1,), (1,)), ((), ()))
F32 = jnp.float32
BF16 = jnp.bfloat16


def listing(got, meta_ref, posb, valb):
    lane = lax.broadcasted_iota(jnp.int32, (DEVS, 128), 1)
    subl = lax.broadcasted_iota(jnp.int32, (DEVS, 128), 0)
    ident = got.astype(F32)
    turned = ident.T
    number = turned.astype(jnp.int32) - 1
    high = lax.shift_right_arithmetic(number, 7)
    low = lax.bitwise_and(number, 127)

    def hot(which, c):
        return jnp.where(subl == which[c : c + 1, :], 1.0, 0.0)

    counts = jnp.zeros((DEVS, 128), F32)
    for c in range(CAP):
        counts = counts + lax.dot_general(
            hot(low, c).astype(BF16), hot(high, c).astype(BF16), NT, preferred_element_type=F32
        )
    counts = counts.astype(BF16)
    named = jnp.zeros((DEVS, 128), F32)
    for c in range(CAP):
        by_low = jnp.dot(counts, hot(high, c).astype(BF16), preferred_element_type=F32)
        times = jnp.sum(by_low * hot(low, c), axis=0, keepdims=True)
        named = jnp.where(subl == c, times, named)
    named = named.T
    first = jnp.where(named == 1.0, 1.0, 0.0).astype(BF16)
    again = jnp.where(named > 1.0, 1.0, 0.0).astype(BF16)
    upper = jnp.where(subl < lane, 1.0, 0.0).astype(BF16)
    lower = jnp.where(lane < subl, 1.0, 0.0).astype(BF16)
    ones = jnp.ones((DEVS, 128), BF16)

    def ranked(flags):
        per_row = jnp.dot(flags, ones, preferred_element_type=F32)
        place = jnp.dot(lower, per_row.astype(BF16), preferred_element_type=F32)
        place = place + jnp.dot(flags, upper, preferred_element_type=F32)
        return place.astype(jnp.int32), jnp.sum(per_row, axis=0, keepdims=True).astype(jnp.int32)

    first_at, first_count = ranked(first)
    again_at, again_count = ranked(again)
    pos = jnp.where(first > 0, first_at, jnp.where(again > 0, LIST * 128 - 1 - again_at, -1))
    value = got + 32768 * (subl * (2 * CAP) + lane)
    for c in range(CAP):
        posb[c] = jnp.broadcast_to(pos[:, c : c + 1], (DEVS, 128))
        valb[c] = jnp.broadcast_to(value[:, c : c + 1], (DEVS, 128))

    def listed(t, carry):
        at = lane + t * 128
        found = jnp.zeros((8, 128), jnp.int32)
        for c in range(CAP):
            hit = jnp.where(posb[c] == at, valb[c], 0)
            found = found + jnp.sum(hit.reshape(DEVS // 8, 8, 128), axis=0)
        found = jnp.sum(found, axis=0, keepdims=True)
        meta_ref[pl.ds(t, 1), :] = jnp.where(found > 0, found - 1, ROWS_DEV)
        return carry

    lax.fori_loop(0, LIST, listed, 0)
    one = lax.broadcasted_iota(jnp.int32, (1, 128), 1)
    meta_ref[pl.ds(LIST, 1), :] = jnp.where(one == 0, first_count, again_count)


def main_kernel(
    q_hbm, k_hbm, pos_ref, owner_ref, row_ref,
    dq_ref, dk_ref, got_ref, meta_ref,
    qbuf, kbuf, sbuf, gbuf, kt, lk, lst, lse, acc, pk, pr, tx, rx, keep,
    keys, ids, got_ids, rows_out, posb, valb,
    lsem, ssem, rsem, st_s, st_r, dq_s, dq_r, ex_s, ex_r, token,
):
    b = lax.axis_index("blk")
    tab = lax.axis_index("table")
    x = lax.div(b, 8)
    me = lax.rem(b, 8)
    z = lax.div(me, 4)
    y = lax.rem(me, 4)
    dev = b * TABLE + tab

    def slot(r, s):
        return 4 * lax.rem(z + s, 2) + lax.rem(y + r, 4)

    def group(p):
        return {"blk": x * 8 + p}

    def along(o):
        return {"blk": lax.rem(x + o, 4) * 8 + me}

    def sibling(o):
        return {"table": lax.rem(tab + o, TABLE)}

    xp, xm = along(1), along(3)
    yp = group(slot(1, 0))
    ym = group(slot(3, 0))
    zp = group(slot(0, 1))

    own_q = pltpu.make_async_copy(q_hbm, qbuf.at[me], lsem.at[0])
    own_k = pltpu.make_async_copy(k_hbm, kbuf.at[0], lsem.at[1])
    own_q.start()
    own_k.start()

    barrier = pltpu.get_barrier_semaphore()
    peers = [group(lax.rem(me + o, 8)) for o in range(1, 8)]
    tables = [sibling(o) for o in range(1, TABLE)]
    for to in peers + [along(o) for o in range(1, 4)] + tables:
        pl.semaphore_signal(barrier, inc=1, device_id=to, device_id_type=MESH)
    pl.semaphore_wait(barrier, 13)
    own_k.wait()
    own_q.wait()

    def half(ref, i, c):
        return ref.at[i, pl.ds(c * H, H)]

    def send(n, src, dst, to):
        copy = pltpu.make_async_remote_copy(
            src_ref=src, dst_ref=dst, send_sem=ssem.at[n], recv_sem=rsem.at[n],
            device_id=to, device_id_type=MESH,
        )
        copy.start()
        return copy

    def arrived(n, ref):
        pltpu.make_async_remote_copy(
            src_ref=ref, dst_ref=ref, send_sem=ssem.at[n], recv_sem=rsem.at[n],
            device_id=xp, device_id_type=MESH,
        ).wait_recv()

    sent = []

    def k_send(n, i, j, c):
        sent.append(send(n, half(kbuf, i, c), half(kbuf, j, c), xp))

    def q_send(n, i, c, to):
        sent.append(send(n, half(qbuf, i, c), half(qbuf, i, c), to))

    k_send(0, 0, 1, 0)
    q_send(4, me, 0, yp)
    q_send(7, me, 1, ym)
    q_send(8, me, 0, zp)
    k_send(1, 0, 1, 1)
    q_send(5, me, 1, yp)
    q_send(6, me, 0, ym)
    q_send(9, me, 1, zp)

    def scores(qi, kind, ks):
        top = jnp.full((8, N), -jnp.inf, F32)
        for t in range(2):
            rows = pl.ds(t * H, H)
            s = lax.dot_general(kbuf[ks, rows, :], qbuf[qi], NT, preferred_element_type=F32)
            sbuf[kind, qi, rows, :] = s
            top = jnp.maximum(top, jnp.max(s.reshape(H // 8, 8, N), axis=0))
        top = jnp.max(top, axis=0, keepdims=True) * C2
        total = jnp.zeros((8, N), F32)
        for t in range(2):
            s = sbuf[kind, qi, pl.ds(t * H, H), :]
            total = total + jnp.sum(jnp.exp2(s * C2 - top).reshape(H // 8, 8, N), axis=0)
        total = jnp.sum(total, axis=0, keepdims=True)
        lk[kind, pl.ds(qi, 1), :] = top + jnp.log(total) * LOG2E

    def mixed_k(qi):
        return jnp.where(qi >= me, 0, 2)

    scores(me, 1, 0)

    owner = owner_ref[...]
    owner_f = owner.astype(F32)
    owner_col = jnp.broadcast_to(owner_f, (8, N)).T[:, 0:1]
    before = lax.broadcasted_iota(jnp.int32, (N, N), 0) < lax.broadcasted_iota(jnp.int32, (N, N), 1)
    rank = jnp.sum(jnp.where((owner_col == owner_f) & before, 1.0, 0.0), axis=0, keepdims=True)
    rank = rank.astype(jnp.int32)
    away = owner - b * TABLE
    away = jnp.where(away < 0, away + DEVS, away)
    keys[...] = away * (2 * CAP) + rank
    row = row_ref[...] + 1
    sub = lax.broadcasted_iota(jnp.int32, (DEVS, N), 0)
    mine = sub == away
    high = jnp.where(mine, (row // 128).astype(F32), 0.0).astype(BF16)
    low = jnp.where(mine, (row % 128).astype(F32), 0.0).astype(BF16)
    place = jnp.where(sub == rank, 1.0, 0.0).astype(BF16)
    message = 128.0 * lax.dot_general(high, place, NT, preferred_element_type=F32)
    message = message + lax.dot_general(low, place, NT, preferred_element_type=F32)
    ids[...] = message.astype(jnp.int32).reshape(DEVS, 1, 128)
    got_ids[dev] = ids[tab]

    for to in tables:
        pl.semaphore_signal(token.at[0], inc=1, device_id=to, device_id_type=MESH)
    pl.semaphore_wait(token.at[0], TABLE - 1)
    for to in peers:
        pl.semaphore_signal(token.at[1], inc=1, device_id=to, device_id_type=MESH)
    pl.semaphore_wait(token.at[1], 7)

    def post(src, dst, n, o, t):
        pltpu.make_async_remote_copy(
            src_ref=src.at[o * TABLE + t], dst_ref=dst.at[dev], send_sem=ex_s.at[n], recv_sem=ex_r.at[n],
            device_id={"blk": lax.rem(b + o, BLK), "table": t}, device_id_type=MESH,
        ).start()

    def post_near(src, dst, n):
        for t in range(TABLE):

            @pl.when(tab != t)
            def _():
                post(src, dst, n, 0, t)

    def tell(o, carry):
        for t in range(TABLE):
            post(ids, got_ids, 0, o, t)
        return carry


    s3, s1, s2, s0 = slot(3, 0), slot(1, 0), slot(2, 0), slot(0, 1)
    t3, t1, t2 = slot(3, 1), slot(1, 1), slot(2, 1)
    arrived(0, half(kbuf, 1, 0))
    k_send(2, 1, 2, 0)
    arrived(4, half(qbuf, s3, 0))
    q_send(10, s3, 0, yp)
    arrived(7, half(qbuf, s1, 1))
    q_send(11, s1, 1, ym)
    arrived(8, half(qbuf, s0, 0))
    q_send(12, s0, 0, yp)
    q_send(14, s0, 0, ym)
    arrived(1, half(kbuf, 1, 1))
    k_send(3, 1, 2, 1)
    arrived(9, half(qbuf, s0, 1))
    q_send(13, s0, 1, yp)
    q_send(15, s0, 1, ym)
    arrived(5, half(qbuf, s3, 1))
    arrived(6, half(qbuf, s1, 0))
    scores(me, 0, 1)

    def first_full(j, carry):
        scores(slot(j + lax.div(j, 2), lax.div(4 - j, 4)), 0, 1)
        return carry

    lax.fori_loop(0, 3, first_full, 0)
    arrived(10, half(qbuf, s2, 0))
    q_send(16, s2, 0, zp)
    arrived(11, half(qbuf, s2, 1))
    q_send(17, s2, 1, zp)
    scores(s2, 0, 1)
    arrived(2, half(kbuf, 2, 0))
    arrived(3, half(kbuf, 2, 1))

    def turn(i, carry):
        kt[i] = kbuf[i].T
        return carry

    lax.fori_loop(0, 3, turn, 0)

    def first_mixed(j, carry):
        qi = slot(j, (4 - j) // 4)
        scores(qi, 1, mixed_k(qi))
        return carry

    lax.fori_loop(0, 4, first_mixed, 0)
    def last_pairs(r):
        qi = slot(r, 1)
        scores(qi, 0, 1)
        scores(qi, 1, mixed_k(qi))

    arrived(12, half(qbuf, t3, 0))
    arrived(13, half(qbuf, t3, 1))
    last_pairs(3)
    arrived(14, half(qbuf, t1, 0))
    arrived(15, half(qbuf, t1, 1))
    last_pairs(1)
    arrived(16, half(qbuf, t2, 0))
    arrived(17, half(qbuf, t2, 1))
    last_pairs(2)

    a, c = lk[0], lk[1]
    top = jnp.maximum(a, c)
    lst[me] = top + jnp.log(jnp.exp2(a - top) + jnp.exp2(c - top)) * LOG2E
    stats = []
    most = pl.ds(0, DEVS - 1)
    for o in range(1, 8):
        copy = pltpu.make_async_remote_copy(
            src_ref=lst.at[me], dst_ref=lst.at[me], send_sem=st_s.at[o - 1], recv_sem=st_r.at[o - 1],
            device_id=group(lax.rem(me + o, 8)), device_id_type=MESH,
        )
        copy.start()
        stats.append(copy)
    post_near(ids, got_ids, 0)
    lax.fori_loop(1, BLK, tell, 0)

    for o in range(1, 8):
        p = lax.rem(me + 8 - o, 8)
        pltpu.make_async_remote_copy(
            src_ref=lst.at[p], dst_ref=lst.at[p], send_sem=st_s.at[o - 1], recv_sem=st_r.at[o - 1],
            device_id=xp, device_id_type=MESH,
        ).wait_recv()
    top = lst[0]
    for i in range(1, 8):
        top = jnp.maximum(top, lst[i])
    total = jnp.exp2(lst[0] - top)
    for i in range(1, 8):
        total = total + jnp.exp2(lst[i] - top)
    lse[...] = top + jnp.log(total) * LOG2E

    def item_rows(kind, qi, t, hot):
        w = jnp.exp2(sbuf[kind, qi, pl.ds(t * H, H), :] * C2 - lse[pl.ds(qi, 1), :])
        if hot:
            places = lax.broadcasted_iota(jnp.int32, (H, N), 0) + t * H
            w = jnp.where(places == pos_ref[...], w - 1.0, w)
        w = w.astype(BF16)
        gbuf[kind, qi, pl.ds(t * H, H), :] = w
        acc[pl.ds(t * H, H), :] += jnp.dot(w, qbuf[qi], preferred_element_type=F32)

    def items_of(kind, lo, hi):
        acc[...] = jnp.zeros((N, D), F32)

        def one(qi, carry):
            for t in range(2):
                item_rows(kind, qi, t, False)
            return carry

        lax.fori_loop(lo, hi, one, 0)

    items_of(1, 0, me)
    pk[0] = acc[...].astype(BF16)
    sent.append(send(18, half(pk, 0, 0), half(pr, 0, 0), xm))
    sent.append(send(19, half(pk, 0, 1), half(pr, 0, 1), xp))
    items_of(0, 0, 8)
    pk[1, pl.ds(H, H), :] = acc[pl.ds(H, H), :].astype(BF16)
    sent.append(send(21, half(pk, 1, 1), half(pr, 1, 1), xm))
    arrived(18, half(pr, 0, 0))
    pk[1, pl.ds(0, H), :] = (acc[pl.ds(0, H), :] + pr[0, pl.ds(0, H), :].astype(F32)).astype(BF16)
    sent.append(send(20, half(pk, 1, 0), half(pr, 1, 0), xm))
    arrived(19, half(pr, 0, 1))
    sent.append(send(22, half(pr, 0, 1), half(pr, 2, 1), xp))
    items_of(1, me + 1, 8)
    for t in range(2):
        item_rows(1, me, t, True)

    def query_part(qi):
        ks = mixed_k(qi)
        part = jnp.dot(kt[1], gbuf[0, qi], preferred_element_type=F32)
        return part + jnp.dot(kt[ks], gbuf[1, qi], preferred_element_type=F32)

    def give(i, h, value, to):
        tx[i, h] = value.astype(BF16)
        copy = pltpu.make_async_remote_copy(
            src_ref=tx.at[i, h], dst_ref=rx.at[i, h], send_sem=dq_s.at[2 * i + h],
            recv_sem=dq_r.at[2 * i + h], device_id=to, device_id_type=MESH,
        )
        copy.start()
        sent.append(copy)

    def given(i, h):
        pltpu.make_async_remote_copy(
            src_ref=rx.at[i, h], dst_ref=rx.at[i, h], send_sem=dq_s.at[2 * i + h],
            recv_sem=dq_r.at[2 * i + h], device_id=xp, device_id_type=MESH,
        ).wait_recv()
        return rx[i, h].astype(F32)

    for i, r, to in ((0, 2, zp), (4, 1, yp), (5, 3, ym)):
        part = query_part(slot(r, 1))
        give(i, 0, part[:, :H], to)
        give(i, 1, part[:, H:], to)
    part = query_part(slot(1, 0))
    give(2, 1, part[:, H:], yp)
    keep[0] = part[:, :H]
    part = query_part(slot(3, 0))
    give(3, 0, part[:, :H], ym)
    keep[1] = part[:, H:]
    part = query_part(slot(0, 1))
    keep[2] = part[:, :H]
    keep[3] = part[:, H:]
    part = query_part(slot(2, 0))
    keep[4] = part[:, :H]
    keep[5] = part[:, H:]
    part = query_part(me)
    keep[6] = part[:, :H]
    keep[7] = part[:, H:]
    give(1, 0, keep[4] + given(0, 0), yp)

    low, high = pl.ds(0, H), pl.ds(H, H)
    arrived(21, half(pr, 1, 1))
    arrived(22, half(pr, 2, 1))
    lower = acc[high, :] + pr[1, high, :].astype(F32) + pr[2, high, :].astype(F32)
    dk_ref[high, :] = (SCALE * lower).astype(BF16)
    arrived(20, half(pr, 1, 0))
    dk_ref[low, :] = (SCALE * (acc[low, :] + pr[1, low, :].astype(F32))).astype(BF16)
    give(1, 1, keep[5] + given(0, 1), ym)

    own = pltpu.make_async_copy(rows_out.at[tab], got_ref.at[dev], lsem.at[2])

    def dispatch(g, carry):
        at = lax.broadcasted_iota(jnp.int32, (16 * 2 * CAP, N), 0) + g * (16 * 2 * CAP)
        left = jnp.where(at == keys[...], 1.0, 0.0).astype(BF16)
        right = jnp.where(at == keys[...] + CAP, 1.0, 0.0).astype(BF16)
        picked = jnp.dot(left, dk_ref[:, 0:128], preferred_element_type=F32)
        picked = picked + jnp.dot(right, dk_ref[:, 128:256], preferred_element_type=F32)
        rows_out[pl.ds(g * 16, 16)] = picked.astype(BF16).reshape(16, 2 * CAP, 128)

        @pl.when(g == 0)
        def _():
            own.start()
            post_near(rows_out, got_ref, 1)

        def four(j, c):
            for t in range(TABLE):
                post(rows_out, got_ref, 1, g * 4 + j, t)
            return c

        lax.fori_loop(jnp.where(g == 0, 1, 0), 4, four, 0)
        return carry

    lax.fori_loop(0, 8, dispatch, 0)

    for h in range(2):
        give(6, h, keep[2 + h] + given(4, h) + given(5, h), zp)
    give(2, 0, keep[0] + given(1, 0), yp)
    give(3, 1, keep[1] + given(1, 1), ym)

    tells = pltpu.make_async_remote_copy(
        src_ref=ids.at[most], dst_ref=got_ids.at[most], send_sem=ex_s.at[0], recv_sem=ex_r.at[0],
        device_id=xp, device_id_type=MESH,
    )
    tells.wait()
    listing(got_ids[...].reshape(DEVS, 128), meta_ref, posb, valb)

    for h in range(2):
        mine = keep[6 + h] + given(2, h) + given(3, h) + given(6, h)
        dq_ref[pl.ds(h * H, H), :] = (SCALE * mine).T.astype(BF16)

    own.wait()
    pltpu.make_async_remote_copy(
        src_ref=rows_out.at[most], dst_ref=got_ref.at[most], send_sem=ex_s.at[1],
        recv_sem=ex_r.at[1], device_id=xp, device_id_type=MESH,
    ).wait()
    for copy in sent:
        copy.wait_send()
    for copy in stats:
        copy.wait_send()


def main_call(queries, items, positives, owner, row):
    vmem = pl.BlockSpec(memory_space=pltpu.VMEM)
    hbm = pl.BlockSpec(memory_space=pl.ANY)
    dma = pltpu.SemaphoreType.DMA
    return pl.pallas_call(
        main_kernel,
        out_shape=(
            jax.ShapeDtypeStruct((N, D), BF16),
            jax.ShapeDtypeStruct((N, D), BF16),
            jax.ShapeDtypeStruct((DEVS, 2 * CAP, 128), BF16),
            jax.ShapeDtypeStruct((LIST + 1, 128), jnp.int32),
        ),
        in_specs=[hbm, hbm, vmem, vmem, vmem],
        out_specs=(vmem, vmem, hbm, vmem),
        scratch_shapes=[
            pltpu.VMEM((8, N, D), BF16),
            pltpu.VMEM((3, N, D), BF16),
            pltpu.VMEM((2, 8, N, N), F32),
            pltpu.VMEM((2, 8, N, N), BF16),
            pltpu.VMEM((3, D, N), BF16),
            pltpu.VMEM((2, 8, N), F32),
            pltpu.VMEM((8, 8, N), F32),
            pltpu.VMEM((8, N), F32),
            pltpu.VMEM((N, D), F32),
            pltpu.VMEM((2, N, D), BF16),
            pltpu.VMEM((3, N, D), BF16),
            pltpu.VMEM((7, 2, D, H), BF16),
            pltpu.VMEM((7, 2, D, H), BF16),
            pltpu.VMEM((8, D, H), F32),
            pltpu.VMEM((1, N), jnp.int32),
            pltpu.VMEM((DEVS, 1, 128), jnp.int32),
            pltpu.VMEM((DEVS, 1, 128), jnp.int32),
            pltpu.VMEM((DEVS, 2 * CAP, 128), BF16),
            pltpu.VMEM((CAP, DEVS, 128), jnp.int32),
            pltpu.VMEM((CAP, DEVS, 128), jnp.int32),
            dma((3,)), dma((23,)), dma((23,)), dma((7,)), dma((7,)), dma((14,)), dma((14,)),
            dma((2,)), dma((2,)), pltpu.SemaphoreType.REGULAR((2,)),
        ],
        compiler_params=pltpu.CompilerParams(
            collective_id=0, has_side_effects=True, vmem_limit_bytes=60 * 1024 * 1024
        ),
        name="band",
    )(queries, items, positives.reshape(1, N), owner.reshape(1, N), row.reshape(1, N))


PIECE = 1024
SLOTS = 8
STEP = 8


def table_kernel(meta, got, out, left, right, rows, stage, sem):
  def clear(i, carry):
      to = pl.ds(pl.multiple_of(i * 512, 512), 512)
      left[to, :] = jnp.zeros((512, 128), F32)
      right[to, :] = jnp.zeros((512, 128), F32)
      return carry
  lax.fori_loop(0, ROWS_DEV // 512, clear, 0)
  def widen(i, carry):
      to = pl.ds(pl.multiple_of(i * 384, 384), 384)
      rows[to, :] = got[pl.ds(i * 16, 16)].astype(F32).reshape(384,128)
      return carry
  lax.fori_loop(0, DEVS // 16, widen, 0)
  def entry(n):
      v = meta[lax.shift_right_logical(n, 7), lax.bitwise_and(n, 127)]
      to = lax.bitwise_and(v, 32767); at = lax.shift_right_logical(v, 15)
      return pl.ds(to, 1), rows[pl.ds(at, 1), :], rows[pl.ds(at + CAP, 1), :]
  def place(i, carry):
      for j in range(STEP):
          to, a, b = entry(i * STEP + j)
          left[to, :] = a
          right[to, :] = b
      return carry
  lax.fori_loop(0, lax.div(meta[LIST, 0] + STEP - 1, STEP), place, 0)
  def again(i, carry):
      for j in range(STEP):
          to, a, b = entry(LIST * 128 - 1 - i * STEP - j)
          left[to, :] += a
          right[to, :] += b
      return carry
  lax.fori_loop(0, lax.div(meta[LIST, 1] + STEP - 1, STEP), again, 0)
  def piece(i):
      at = i * PIECE if isinstance(i, int) else pl.multiple_of(i * PIECE, PIECE)
      return pltpu.make_async_copy(stage.at[lax.rem(i, SLOTS)], out.at[pl.ds(at, PIECE)], sem.at[lax.rem(i, SLOTS)])
  def store(i, carry):
      @pl.when(i >= SLOTS)
      def _():
          piece(i - SLOTS).wait()
      s = lax.rem(i, SLOTS)
      def turn(j, carry):
          at = pl.ds(pl.multiple_of(i * PIECE + j * 256, 256), 256)
          to = pl.ds(pl.multiple_of(j * 256, 256), 256)
          stage[s, to, 0:128] = left[at, :].astype(BF16)
          stage[s, to, 128:256] = right[at, :].astype(BF16)
          return carry
      lax.fori_loop(0, PIECE // 256, turn, 0)
      piece(i).start()
      return carry
  pieces = ROWS_DEV // PIECE
  lax.fori_loop(0, pieces, store, 0)
  for k in range(SLOTS): piece(pieces - SLOTS + k).wait()


def table_call(meta, got):
    return pl.pallas_call(
        table_kernel,
        out_shape=jax.ShapeDtypeStruct((ROWS_DEV, D), BF16),
        in_specs=[pl.BlockSpec(memory_space=pltpu.SMEM), pl.BlockSpec(memory_space=pltpu.VMEM)],
        out_specs=pl.BlockSpec(memory_space=pl.ANY),
        scratch_shapes=[
            pltpu.VMEM((ROWS_DEV + 8, 128), F32),
            pltpu.VMEM((ROWS_DEV + 8, 128), F32),
            pltpu.VMEM((DEVS * 2 * CAP, 128), F32),
            pltpu.VMEM((SLOTS, PIECE, D), BF16),
            pltpu.SemaphoreType.DMA((SLOTS,)),
        ],
        compiler_params=pltpu.CompilerParams(vmem_limit_bytes=60 * 1024 * 1024),
        name="table",
    )(meta, got)


def local(queries, items, positives, item_owner, item_row):
    query_grad, item_grad, got, meta = main_call(queries, items, positives, item_owner, item_row)
    return (query_grad, item_grad, table_call(meta, got))


def solution(mesh):
    in_specs = (
        P(("blk", "table"), None),
        P(("blk", "table"), None),
        P(("blk", "table")),
        P(("blk", "table"), None),
        P(("blk", "table")),
    )
    out_specs = (P(("blk", "table"), None), P(("blk", "table"), None), P(("blk", "table"), None))
    return jax.shard_map(local, mesh=mesh, in_specs=in_specs, out_specs=out_specs, check_vma=False)
```

```python
import math

import jax
import jax.numpy as jnp
from jax import lax
from jax.experimental import pallas as pl
from jax.experimental.pallas import tpu as pltpu
from jax.sharding import PartitionSpec as P

ROWS_DEV = 16384
N = 512
D = 256
H = 256
DEVS = 128
TABLE = 4
CAP = 12
BLK = 32
LIST = 13
SCALE = 3.0 / math.sqrt(D)
LOG2E = 1.4426950408889634
C2 = SCALE * LOG2E
MESH = pl.DeviceIdType.MESH
NT = (((1,), (1,)), ((), ()))
F32 = jnp.float32
BF16 = jnp.bfloat16


def listing(got, meta_ref, posb, valb):
    lane = lax.broadcasted_iota(jnp.int32, (DEVS, 128), 1)
    subl = lax.broadcasted_iota(jnp.int32, (DEVS, 128), 0)
    ident = got.astype(F32)
    turned = ident.T
    number = turned.astype(jnp.int32) - 1
    high = lax.shift_right_arithmetic(number, 7)
    low = lax.bitwise_and(number, 127)

    def hot(which, c):
        return jnp.where(subl == which[c : c + 1, :], 1.0, 0.0)

    counts = jnp.zeros((DEVS, 128), F32)
    for c in range(CAP):
        counts = counts + lax.dot_general(
            hot(low, c).astype(BF16), hot(high, c).astype(BF16), NT, preferred_element_type=F32
        )
    counts = counts.astype(BF16)
    named = jnp.zeros((DEVS, 128), F32)
    for c in range(CAP):
        by_low = jnp.dot(counts, hot(high, c).astype(BF16), preferred_element_type=F32)
        times = jnp.sum(by_low * hot(low, c), axis=0, keepdims=True)
        named = jnp.where(subl == c, times, named)
    named = named.T
    first = jnp.where(named == 1.0, 1.0, 0.0).astype(BF16)
    again = jnp.where(named > 1.0, 1.0, 0.0).astype(BF16)
    upper = jnp.where(subl < lane, 1.0, 0.0).astype(BF16)
    lower = jnp.where(lane < subl, 1.0, 0.0).astype(BF16)
    ones = jnp.ones((DEVS, 128), BF16)

    def ranked(flags):
        per_row = jnp.dot(flags, ones, preferred_element_type=F32)
        place = jnp.dot(lower, per_row.astype(BF16), preferred_element_type=F32)
        place = place + jnp.dot(flags, upper, preferred_element_type=F32)
        return place.astype(jnp.int32), jnp.sum(per_row, axis=0, keepdims=True).astype(jnp.int32)

    first_at, first_count = ranked(first)
    again_at, again_count = ranked(again)
    pos = jnp.where(first > 0, first_at, jnp.where(again > 0, LIST * 128 - 1 - again_at, -1))
    value = got + 32768 * (subl * (2 * CAP) + lane)
    for c in range(CAP):
        posb[c] = jnp.broadcast_to(pos[:, c : c + 1], (DEVS, 128))
        valb[c] = jnp.broadcast_to(value[:, c : c + 1], (DEVS, 128))

    def listed(t, carry):
        at = lane + t * 128
        found = jnp.zeros((8, 128), jnp.int32)
        for c in range(CAP):
            hit = jnp.where(posb[c] == at, valb[c], 0)
            found = found + jnp.sum(hit.reshape(DEVS // 8, 8, 128), axis=0)
        found = jnp.sum(found, axis=0, keepdims=True)
        meta_ref[pl.ds(t, 1), :] = jnp.where(found > 0, found - 1, ROWS_DEV)
        return carry

    lax.fori_loop(0, LIST, listed, 0)
    one = lax.broadcasted_iota(jnp.int32, (1, 128), 1)
    meta_ref[pl.ds(LIST, 1), :] = jnp.where(one == 0, first_count, again_count)


def main_kernel(
    q_hbm, k_hbm, pos_ref, owner_ref, row_ref,
    dq_ref, dk_ref, got_ref, meta_ref,
    qbuf, kbuf, sbuf, gbuf, kt, lk, lst, lse, acc, pk, pr, tx, rx, keep,
    keys, ids, got_ids, rows_out, posb, valb,
    lsem, ssem, rsem, st_s, st_r, dq_s, dq_r, ex_s, ex_r, token,
):
    b = lax.axis_index("blk")
    tab = lax.axis_index("table")
    x = lax.div(b, 8)
    me = lax.rem(b, 8)
    z = lax.div(me, 4)
    y = lax.rem(me, 4)
    dev = b * TABLE + tab

    def slot(r, s):
        return 4 * lax.rem(z + s, 2) + lax.rem(y + r, 4)

    def group(p):
        return {"blk": x * 8 + p}

    def along(o):
        return {"blk": lax.rem(x + o, 4) * 8 + me}

    def sibling(o):
        return {"table": lax.rem(tab + o, TABLE)}

    xp, xm = along(1), along(3)
    yp = group(slot(1, 0))
    ym = group(slot(3, 0))
    zp = group(slot(0, 1))

    own_q = pltpu.make_async_copy(q_hbm, qbuf.at[me], lsem.at[0])
    own_k = pltpu.make_async_copy(k_hbm, kbuf.at[0], lsem.at[1])
    own_q.start()
    own_k.start()

    barrier = pltpu.get_barrier_semaphore()
    peers = [group(lax.rem(me + o, 8)) for o in range(1, 8)]
    tables = [sibling(o) for o in range(1, TABLE)]
    for to in peers + [along(o) for o in range(1, 4)] + tables:
        pl.semaphore_signal(barrier, inc=1, device_id=to, device_id_type=MESH)
    pl.semaphore_wait(barrier, 13)
    own_k.wait()
    own_q.wait()

    def half(ref, i, c):
        return ref.at[i, pl.ds(c * H, H)]

    def send(n, src, dst, to):
        copy = pltpu.make_async_remote_copy(
            src_ref=src, dst_ref=dst, send_sem=ssem.at[n], recv_sem=rsem.at[n],
            device_id=to, device_id_type=MESH,
        )
        copy.start()
        return copy

    def arrived(n, ref):
        pltpu.make_async_remote_copy(
            src_ref=ref, dst_ref=ref, send_sem=ssem.at[n], recv_sem=rsem.at[n],
            device_id=xp, device_id_type=MESH,
        ).wait_recv()

    sent = []

    def k_send(n, i, j, c):
        sent.append(send(n, half(kbuf, i, c), half(kbuf, j, c), xp))

    def q_send(n, i, c, to):
        sent.append(send(n, half(qbuf, i, c), half(qbuf, i, c), to))

    def quarter(i, k):
        return qbuf.at[i, pl.ds(k * (H // 2), H // 2)]

    def quarter_send(n, i, k, to):
        sent.append(send(n, quarter(i, k), quarter(i, k), to))

    k_send(0, 0, 1, 0)
    quarter_send(4, me, 0, yp)
    quarter_send(7, me, 2, ym)
    q_send(8, me, 0, zp)
    quarter_send(23, me, 1, yp)
    quarter_send(24, me, 3, ym)
    k_send(1, 0, 1, 1)
    q_send(9, me, 1, zp)

    def scores(qi, kind, ks):
        top = jnp.full((8, N), -jnp.inf, F32)
        for t in range(2):
            rows = pl.ds(t * H, H)
            s = lax.dot_general(kbuf[ks, rows, :], qbuf[qi], NT, preferred_element_type=F32)
            sbuf[kind, qi, rows, :] = s
            top = jnp.maximum(top, jnp.max(s.reshape(H // 8, 8, N), axis=0))
        top = jnp.max(top, axis=0, keepdims=True) * C2
        total = jnp.zeros((8, N), F32)
        for t in range(2):
            s = sbuf[kind, qi, pl.ds(t * H, H), :]
            total = total + jnp.sum(jnp.exp2(s * C2 - top).reshape(H // 8, 8, N), axis=0)
        total = jnp.sum(total, axis=0, keepdims=True)
        lk[kind, pl.ds(qi, 1), :] = top + jnp.log(total) * LOG2E

    def mixed_k(qi):
        return jnp.where(qi >= me, 0, 2)

    scores(me, 1, 0)

    owner = owner_ref[...]
    owner_f = owner.astype(F32)
    owner_col = jnp.broadcast_to(owner_f, (8, N)).T[:, 0:1]
    before = lax.broadcasted_iota(jnp.int32, (N, N), 0) < lax.broadcasted_iota(jnp.int32, (N, N), 1)
    rank = jnp.sum(jnp.where((owner_col == owner_f) & before, 1.0, 0.0), axis=0, keepdims=True)
    rank = rank.astype(jnp.int32)
    away = owner - b * TABLE
    away = jnp.where(away < 0, away + DEVS, away)
    keys[...] = away * (2 * CAP) + rank
    row = row_ref[...] + 1
    sub = lax.broadcasted_iota(jnp.int32, (DEVS, N), 0)
    mine = sub == away
    high = jnp.where(mine, (row // 128).astype(F32), 0.0).astype(BF16)
    low = jnp.where(mine, (row % 128).astype(F32), 0.0).astype(BF16)
    place = jnp.where(sub == rank, 1.0, 0.0).astype(BF16)
    message = 128.0 * lax.dot_general(high, place, NT, preferred_element_type=F32)
    message = message + lax.dot_general(low, place, NT, preferred_element_type=F32)
    ids[...] = message.astype(jnp.int32).reshape(DEVS, 1, 128)
    got_ids[dev] = ids[tab]

    for to in tables:
        pl.semaphore_signal(token.at[0], inc=1, device_id=to, device_id_type=MESH)
    pl.semaphore_wait(token.at[0], TABLE - 1)
    for to in peers:
        pl.semaphore_signal(token.at[1], inc=1, device_id=to, device_id_type=MESH)
    pl.semaphore_wait(token.at[1], 7)

    def post(src, dst, n, o, t):
        pltpu.make_async_remote_copy(
            src_ref=src.at[o * TABLE + t], dst_ref=dst.at[dev], send_sem=ex_s.at[n], recv_sem=ex_r.at[n],
            device_id={"blk": lax.rem(b + o, BLK), "table": t}, device_id_type=MESH,
        ).start()

    def post_near(src, dst, n):
        for t in range(TABLE):

            @pl.when(tab != t)
            def _():
                post(src, dst, n, 0, t)

    def tell(o, carry):
        for t in range(TABLE):
            post(ids, got_ids, 0, o, t)
        return carry


    s3, s1, s2, s0 = slot(3, 0), slot(1, 0), slot(2, 0), slot(0, 1)
    t3, t1, t2 = slot(3, 1), slot(1, 1), slot(2, 1)
    arrived(4, quarter(s3, 0))
    quarter_send(10, s3, 0, yp)
    arrived(7, quarter(s1, 2))
    quarter_send(11, s1, 2, ym)
    arrived(0, half(kbuf, 1, 0))
    k_send(2, 1, 2, 0)
    arrived(23, quarter(s3, 1))
    quarter_send(25, s3, 1, yp)
    q_send(5, me, 1, yp)
    arrived(24, quarter(s1, 3))
    quarter_send(26, s1, 3, ym)
    q_send(6, me, 0, ym)
    arrived(8, half(qbuf, s0, 0))
    q_send(12, s0, 0, yp)
    q_send(14, s0, 0, ym)
    arrived(1, half(kbuf, 1, 1))
    k_send(3, 1, 2, 1)
    arrived(9, half(qbuf, s0, 1))
    q_send(13, s0, 1, yp)
    q_send(15, s0, 1, ym)
    for arrival, n, k in ((10, 16, 0), (11, 17, 2), (25, 27, 1), (26, 28, 3)):
        arrived(arrival, quarter(s2, k))
        quarter_send(n, s2, k, zp)
    post_near(ids, got_ids, 0)
    lax.fori_loop(1, 11, tell, 0)
    scores(me, 0, 1)

    def early_full(j, carry):
        scores(slot(2 * j, 1 - j), 0, 1)
        return carry

    lax.fori_loop(0, 2, early_full, 0)
    arrived(5, half(qbuf, s3, 1))
    arrived(6, half(qbuf, s1, 0))

    def late_full(j, carry):
        scores(slot(2 * j + 1, 0), 0, 1)
        return carry

    lax.fori_loop(0, 2, late_full, 0)
    lax.fori_loop(11, 22, tell, 0)
    arrived(2, half(kbuf, 2, 0))
    arrived(3, half(kbuf, 2, 1))

    def turn(i, carry):
        kt[i] = kbuf[i].T
        return carry

    lax.fori_loop(0, 3, turn, 0)

    def first_mixed(j, carry):
        qi = slot(j, lax.div(4 - j, 4))
        scores(qi, 1, mixed_k(qi))
        return carry

    lax.fori_loop(0, 4, first_mixed, 0)
    lax.fori_loop(22, BLK, tell, 0)

    def last_pairs(r):
        qi = slot(r, 1)
        scores(qi, 0, 1)
        scores(qi, 1, mixed_k(qi))

    arrived(12, half(qbuf, t3, 0))
    arrived(13, half(qbuf, t3, 1))
    last_pairs(3)
    arrived(14, half(qbuf, t1, 0))
    arrived(15, half(qbuf, t1, 1))
    last_pairs(1)
    for n, k in ((16, 0), (17, 2), (27, 1), (28, 3)):
        arrived(n, quarter(t2, k))
    last_pairs(2)

    a, c = lk[0], lk[1]
    top = jnp.maximum(a, c)
    lst[me] = top + jnp.log(jnp.exp2(a - top) + jnp.exp2(c - top)) * LOG2E
    stats = []
    most = pl.ds(0, DEVS - 1)
    for o in range(1, 8):
        copy = pltpu.make_async_remote_copy(
            src_ref=lst.at[me], dst_ref=lst.at[me], send_sem=st_s.at[o - 1], recv_sem=st_r.at[o - 1],
            device_id=group(lax.rem(me + o, 8)), device_id_type=MESH,
        )
        copy.start()
        stats.append(copy)

    for o in range(1, 8):
        p = lax.rem(me + 8 - o, 8)
        pltpu.make_async_remote_copy(
            src_ref=lst.at[p], dst_ref=lst.at[p], send_sem=st_s.at[o - 1], recv_sem=st_r.at[o - 1],
            device_id=xp, device_id_type=MESH,
        ).wait_recv()
    top = lst[0]
    for i in range(1, 8):
        top = jnp.maximum(top, lst[i])
    total = jnp.exp2(lst[0] - top)
    for i in range(1, 8):
        total = total + jnp.exp2(lst[i] - top)
    lse[...] = top + jnp.log(total) * LOG2E

    def item_rows(kind, qi, t, hot):
        w = jnp.exp2(sbuf[kind, qi, pl.ds(t * H, H), :] * C2 - lse[pl.ds(qi, 1), :])
        if hot:
            places = lax.broadcasted_iota(jnp.int32, (H, N), 0) + t * H
            w = jnp.where(places == pos_ref[...], w - 1.0, w)
        w = w.astype(BF16)
        gbuf[kind, qi, pl.ds(t * H, H), :] = w
        acc[pl.ds(t * H, H), :] += jnp.dot(w, qbuf[qi], preferred_element_type=F32)

    def items_of(kind, lo, hi):
        acc[...] = jnp.zeros((N, D), F32)

        def one(qi, carry):
            for t in range(2):
                item_rows(kind, qi, t, False)
            return carry

        lax.fori_loop(lo, hi, one, 0)

    items_of(1, 0, me)
    pk[0] = acc[...].astype(BF16)
    sent.append(send(18, half(pk, 0, 0), half(pr, 0, 0), xm))
    sent.append(send(19, half(pk, 0, 1), half(pr, 0, 1), xp))
    items_of(0, 0, 8)
    pk[1, pl.ds(H, H), :] = acc[pl.ds(H, H), :].astype(BF16)
    sent.append(send(21, half(pk, 1, 1), half(pr, 1, 1), xm))
    arrived(18, half(pr, 0, 0))
    pk[1, pl.ds(0, H), :] = (acc[pl.ds(0, H), :] + pr[0, pl.ds(0, H), :].astype(F32)).astype(BF16)
    sent.append(send(20, half(pk, 1, 0), half(pr, 1, 0), xm))
    arrived(19, half(pr, 0, 1))
    sent.append(send(22, half(pr, 0, 1), half(pr, 2, 1), xp))
    items_of(1, me + 1, 8)
    for t in range(2):
        item_rows(1, me, t, True)

    def query_part(qi):
        ks = mixed_k(qi)
        part = jnp.dot(kt[1], gbuf[0, qi], preferred_element_type=F32)
        return part + jnp.dot(kt[ks], gbuf[1, qi], preferred_element_type=F32)

    def give(i, h, value, to):
        tx[i, h] = value.astype(BF16)
        copy = pltpu.make_async_remote_copy(
            src_ref=tx.at[i, h], dst_ref=rx.at[i, h], send_sem=dq_s.at[2 * i + h],
            recv_sem=dq_r.at[2 * i + h], device_id=to, device_id_type=MESH,
        )
        copy.start()
        sent.append(copy)

    def given(i, h):
        pltpu.make_async_remote_copy(
            src_ref=rx.at[i, h], dst_ref=rx.at[i, h], send_sem=dq_s.at[2 * i + h],
            recv_sem=dq_r.at[2 * i + h], device_id=xp, device_id_type=MESH,
        ).wait_recv()
        return rx[i, h].astype(F32)

    for i, r, to in ((0, 2, zp), (4, 1, yp), (5, 3, ym)):
        part = query_part(slot(r, 1))
        give(i, 0, part[:, :H], to)
        give(i, 1, part[:, H:], to)
    part = query_part(slot(1, 0))
    give(2, 1, part[:, H:], yp)
    keep[0] = part[:, :H]
    part = query_part(slot(3, 0))
    give(3, 0, part[:, :H], ym)
    keep[1] = part[:, H:]
    part = query_part(slot(0, 1))
    keep[2] = part[:, :H]
    keep[3] = part[:, H:]
    part = query_part(slot(2, 0))
    keep[4] = part[:, :H]
    keep[5] = part[:, H:]
    part = query_part(me)
    keep[6] = part[:, :H]
    keep[7] = part[:, H:]
    give(1, 0, keep[4] + given(0, 0), yp)

    low, high = pl.ds(0, H), pl.ds(H, H)
    arrived(21, half(pr, 1, 1))
    arrived(22, half(pr, 2, 1))
    lower = acc[high, :] + pr[1, high, :].astype(F32) + pr[2, high, :].astype(F32)
    dk_ref[high, :] = (SCALE * lower).astype(BF16)
    arrived(20, half(pr, 1, 0))
    dk_ref[low, :] = (SCALE * (acc[low, :] + pr[1, low, :].astype(F32))).astype(BF16)
    give(1, 1, keep[5] + given(0, 1), ym)

    own = pltpu.make_async_copy(rows_out.at[tab], got_ref.at[dev], lsem.at[2])

    def dispatch(g, carry):
        at = lax.broadcasted_iota(jnp.int32, (16 * 2 * CAP, N), 0) + g * (16 * 2 * CAP)
        left = jnp.where(at == keys[...], 1.0, 0.0).astype(BF16)
        right = jnp.where(at == keys[...] + CAP, 1.0, 0.0).astype(BF16)
        picked = jnp.dot(left, dk_ref[:, 0:128], preferred_element_type=F32)
        picked = picked + jnp.dot(right, dk_ref[:, 128:256], preferred_element_type=F32)
        rows_out[pl.ds(g * 16, 16)] = picked.astype(BF16).reshape(16, 2 * CAP, 128)

        @pl.when(g == 0)
        def _():
            own.start()
            post_near(rows_out, got_ref, 1)

        def four(j, c):
            for t in range(TABLE):
                post(rows_out, got_ref, 1, g * 4 + j, t)
            return c

        lax.fori_loop(jnp.where(g == 0, 1, 0), 4, four, 0)
        return carry

    lax.fori_loop(0, 8, dispatch, 0)

    for h in range(2):
        give(6, h, keep[2 + h] + given(4, h) + given(5, h), zp)
    give(2, 0, keep[0] + given(1, 0), yp)
    give(3, 1, keep[1] + given(1, 1), ym)

    tells = pltpu.make_async_remote_copy(
        src_ref=ids.at[most], dst_ref=got_ids.at[most], send_sem=ex_s.at[0], recv_sem=ex_r.at[0],
        device_id=xp, device_id_type=MESH,
    )
    tells.wait()
    listing(got_ids[...].reshape(DEVS, 128), meta_ref, posb, valb)

    for h in range(2):
        mine = keep[6 + h] + given(2, h) + given(3, h) + given(6, h)
        dq_ref[pl.ds(h * H, H), :] = (SCALE * mine).T.astype(BF16)

    own.wait()
    pltpu.make_async_remote_copy(
        src_ref=rows_out.at[most], dst_ref=got_ref.at[most], send_sem=ex_s.at[1],
        recv_sem=ex_r.at[1], device_id=xp, device_id_type=MESH,
    ).wait()
    for copy in sent:
        copy.wait_send()
    for copy in stats:
        copy.wait_send()


def main_call(queries, items, positives, owner, row):
    vmem = pl.BlockSpec(memory_space=pltpu.VMEM)
    hbm = pl.BlockSpec(memory_space=pl.ANY)
    dma = pltpu.SemaphoreType.DMA
    return pl.pallas_call(
        main_kernel,
        out_shape=(
            jax.ShapeDtypeStruct((N, D), BF16),
            jax.ShapeDtypeStruct((N, D), BF16),
            jax.ShapeDtypeStruct((DEVS, 2 * CAP, 128), BF16),
            jax.ShapeDtypeStruct((LIST + 1, 128), jnp.int32),
        ),
        in_specs=[hbm, hbm, vmem, vmem, vmem],
        out_specs=(vmem, vmem, hbm, vmem),
        scratch_shapes=[
            pltpu.VMEM((8, N, D), BF16),
            pltpu.VMEM((3, N, D), BF16),
            pltpu.VMEM((2, 8, N, N), F32),
            pltpu.VMEM((2, 8, N, N), BF16),
            pltpu.VMEM((3, D, N), BF16),
            pltpu.VMEM((2, 8, N), F32),
            pltpu.VMEM((8, 8, N), F32),
            pltpu.VMEM((8, N), F32),
            pltpu.VMEM((N, D), F32),
            pltpu.VMEM((2, N, D), BF16),
            pltpu.VMEM((3, N, D), BF16),
            pltpu.VMEM((7, 2, D, H), BF16),
            pltpu.VMEM((7, 2, D, H), BF16),
            pltpu.VMEM((8, D, H), F32),
            pltpu.VMEM((1, N), jnp.int32),
            pltpu.VMEM((DEVS, 1, 128), jnp.int32),
            pltpu.VMEM((DEVS, 1, 128), jnp.int32),
            pltpu.VMEM((DEVS, 2 * CAP, 128), BF16),
            pltpu.VMEM((CAP, DEVS, 128), jnp.int32),
            pltpu.VMEM((CAP, DEVS, 128), jnp.int32),
            dma((3,)), dma((29,)), dma((29,)), dma((7,)), dma((7,)), dma((14,)), dma((14,)),
            dma((2,)), dma((2,)), pltpu.SemaphoreType.REGULAR((2,)),
        ],
        compiler_params=pltpu.CompilerParams(
            collective_id=0, has_side_effects=True, vmem_limit_bytes=60 * 1024 * 1024
        ),
        name="band",
    )(queries, items, positives.reshape(1, N), owner.reshape(1, N), row.reshape(1, N))


PIECE = 1024
SLOTS = 8
STEP = 16


def table_kernel(
    meta, got_hbm, dq_in, dk_in, out, dq_out, dk_out, left, right, rows, stage, got, kept, sem, load_sem
):
    loads = [
        pltpu.make_async_copy(got_hbm, got, load_sem.at[0]),
        pltpu.make_async_copy(dq_in, kept.at[0], load_sem.at[1]),
        pltpu.make_async_copy(dk_in, kept.at[1], load_sem.at[2]),
    ]
    for copy in loads:
        copy.start()

    def clear(i, carry):
        to = pl.ds(pl.multiple_of(i * 512, 512), 512)
        left[to, :] = jnp.zeros((512, 128), F32)
        right[to, :] = jnp.zeros((512, 128), F32)
        return carry

    lax.fori_loop(0, ROWS_DEV // 512, clear, 0)
    for copy in loads:
        copy.wait()
    passed = [
        pltpu.make_async_copy(kept.at[0], dq_out, load_sem.at[3]),
        pltpu.make_async_copy(kept.at[1], dk_out, load_sem.at[4]),
    ]
    for copy in passed:
        copy.start()

    def widen(i, carry):
        to = pl.ds(pl.multiple_of(i * 384, 384), 384)
        rows[to, :] = got[pl.ds(i * 16, 16)].astype(F32).reshape(384, 128)
        return carry

    lax.fori_loop(0, DEVS // 16, widen, 0)

    def entry(n):
        v = meta[lax.shift_right_logical(n, 7), lax.bitwise_and(n, 127)]
        at = lax.shift_right_logical(v, 15)
        return pl.ds(lax.bitwise_and(v, 32767), 1), rows[pl.ds(at, 1), :], rows[pl.ds(at + CAP, 1), :]

    def place(i, carry):
        for to, a, b in [entry(i * STEP + j) for j in range(STEP)]:
            left[to, :] = a
            right[to, :] = b
        return carry

    lax.fori_loop(0, lax.div(meta[LIST, 0] + STEP - 1, STEP), place, 0)

    def again(i, carry):
        for j in range(STEP):
            to, a, b = entry(LIST * 128 - 1 - i * STEP - j)
            left[to, :] += a
            right[to, :] += b
        return carry

    lax.fori_loop(0, lax.div(meta[LIST, 1] + STEP - 1, STEP), again, 0)

    def piece(i):
        at = i * PIECE if isinstance(i, int) else pl.multiple_of(i * PIECE, PIECE)
        k = lax.rem(i, SLOTS)
        return pltpu.make_async_copy(stage.at[k], out.at[pl.ds(at, PIECE)], sem.at[k])

    def store(i, carry):
        @pl.when(i >= SLOTS)
        def _():
            piece(i - SLOTS).wait()

        k = lax.rem(i, SLOTS)

        def turn(j, c):
            at = pl.ds(pl.multiple_of(i * PIECE + j * 256, 256), 256)
            to = pl.ds(pl.multiple_of(j * 256, 256), 256)
            stage[k, to, 0:128] = left[at, :].astype(BF16)
            stage[k, to, 128:256] = right[at, :].astype(BF16)
            return c

        lax.fori_loop(0, PIECE // 256, turn, 0)
        piece(i).start()
        return carry

    pieces = ROWS_DEV // PIECE
    lax.fori_loop(0, pieces, store, 0)
    for i in range(pieces - SLOTS, pieces):
        piece(i).wait()
    for copy in passed:
        copy.wait()


def table_call(meta, got, query_grad, item_grad):
    hbm = pl.BlockSpec(memory_space=pl.ANY)
    grad = jax.ShapeDtypeStruct((N, D), BF16)
    return pl.pallas_call(
        table_kernel,
        out_shape=(jax.ShapeDtypeStruct((ROWS_DEV, D), BF16), grad, grad),
        in_specs=[pl.BlockSpec(memory_space=pltpu.SMEM), hbm, hbm, hbm],
        out_specs=(hbm, hbm, hbm),
        scratch_shapes=[
            pltpu.VMEM((ROWS_DEV + 8, 128), F32),
            pltpu.VMEM((ROWS_DEV + 8, 128), F32),
            pltpu.VMEM((DEVS * 2 * CAP, 128), F32),
            pltpu.VMEM((SLOTS, PIECE, D), BF16),
            pltpu.VMEM((DEVS, 2 * CAP, 128), BF16),
            pltpu.VMEM((2, N, D), BF16),
            pltpu.SemaphoreType.DMA((SLOTS,)),
            pltpu.SemaphoreType.DMA((5,)),
        ],
        compiler_params=pltpu.CompilerParams(vmem_limit_bytes=60 * 1024 * 1024),
        name="table",
    )(meta, got, query_grad, item_grad)


def local(queries, items, positives, item_owner, item_row):
    query_grad, item_grad, got, meta = main_call(queries, items, positives, item_owner, item_row)
    table_grad, query_grad, item_grad = table_call(meta, got, query_grad, item_grad)
    return (query_grad, item_grad, table_grad)


def solution(mesh):
    in_specs = (
        P(("blk", "table"), None),
        P(("blk", "table"), None),
        P(("blk", "table")),
        P(("blk", "table"), None),
        P(("blk", "table")),
    )
    out_specs = (P(("blk", "table"), None), P(("blk", "table"), None), P(("blk", "table"), None))
    return jax.shard_map(local, mesh=mesh, in_specs=in_specs, out_specs=out_specs, check_vma=False)
```

```python
import math

import jax
import jax.numpy as jnp
from jax import lax
from jax.experimental import pallas as pl
from jax.experimental.pallas import tpu as pltpu
from jax.sharding import PartitionSpec as P

ROWS_DEV = 16384
N = 512
D = 256
H = 256
DEVS = 128
TABLE = 4
CAP = 12
BLK = 32
LIST = 13
SCALE = 3.0 / math.sqrt(D)
LOG2E = 1.4426950408889634
C2 = SCALE * LOG2E
MESH = pl.DeviceIdType.MESH
NT = (((1,), (1,)), ((), ()))
F32 = jnp.float32
BF16 = jnp.bfloat16


def listing(got, meta_ref, posb, valb):
    lane = lax.broadcasted_iota(jnp.int32, (DEVS, 128), 1)
    subl = lax.broadcasted_iota(jnp.int32, (DEVS, 128), 0)
    ident = got.astype(F32)
    turned = ident.T
    number = turned.astype(jnp.int32) - 1
    high = lax.shift_right_arithmetic(number, 7)
    low = lax.bitwise_and(number, 127)

    def hot(which, c):
        return jnp.where(subl == which[c : c + 1, :], 1.0, 0.0)

    counts = jnp.zeros((DEVS, 128), F32)
    for c in range(CAP):
        counts = counts + lax.dot_general(
            hot(low, c).astype(BF16), hot(high, c).astype(BF16), NT, preferred_element_type=F32
        )
    counts = counts.astype(BF16)
    named = jnp.zeros((DEVS, 128), F32)
    for c in range(CAP):
        by_low = jnp.dot(counts, hot(high, c).astype(BF16), preferred_element_type=F32)
        times = jnp.sum(by_low * hot(low, c), axis=0, keepdims=True)
        named = jnp.where(subl == c, times, named)
    named = named.T
    first = jnp.where(named == 1.0, 1.0, 0.0).astype(BF16)
    again = jnp.where(named > 1.0, 1.0, 0.0).astype(BF16)
    upper = jnp.where(subl < lane, 1.0, 0.0).astype(BF16)
    lower = jnp.where(lane < subl, 1.0, 0.0).astype(BF16)
    ones = jnp.ones((DEVS, 128), BF16)

    def ranked(flags):
        per_row = jnp.dot(flags, ones, preferred_element_type=F32)
        place = jnp.dot(lower, per_row.astype(BF16), preferred_element_type=F32)
        place = place + jnp.dot(flags, upper, preferred_element_type=F32)
        return place.astype(jnp.int32), jnp.sum(per_row, axis=0, keepdims=True).astype(jnp.int32)

    first_at, first_count = ranked(first)
    again_at, again_count = ranked(again)
    pos = jnp.where(first > 0, first_at, jnp.where(again > 0, LIST * 128 - 1 - again_at, -1))
    value = got + 32768 * (subl * (2 * CAP) + lane)
    for c in range(CAP):
        posb[c] = jnp.broadcast_to(pos[:, c : c + 1], (DEVS, 128))
        valb[c] = jnp.broadcast_to(value[:, c : c + 1], (DEVS, 128))

    def listed(t, carry):
        at = lane + t * 128
        found = jnp.zeros((8, 128), jnp.int32)
        for c in range(CAP):
            hit = jnp.where(posb[c] == at, valb[c], 0)
            found = found + jnp.sum(hit.reshape(DEVS // 8, 8, 128), axis=0)
        found = jnp.sum(found, axis=0, keepdims=True)
        meta_ref[pl.ds(t, 1), :] = jnp.where(found > 0, found - 1, ROWS_DEV)
        return carry

    lax.fori_loop(0, LIST, listed, 0)
    one = lax.broadcasted_iota(jnp.int32, (1, 128), 1)
    meta_ref[pl.ds(LIST, 1), :] = jnp.where(one == 0, first_count, again_count)


def main_kernel(
    q_hbm, k_hbm, pos_ref, owner_ref, row_ref,
    dq_ref, dk_ref, got_ref, meta_ref,
    qbuf, kbuf, sbuf, gbuf, kt, lk, lst, lse, acc, pk, pr, tx, rx, keep,
    keys, ids, got_ids, rows_out, posb, valb,
    lsem, ssem, rsem, st_s, st_r, dq_s, dq_r, ex_s, ex_r, token,
):
    b = lax.axis_index("blk")
    tab = lax.axis_index("table")
    x = lax.div(b, 8)
    me = lax.rem(b, 8)
    z = lax.div(me, 4)
    y = lax.rem(me, 4)
    dev = b * TABLE + tab

    def slot(r, s):
        return 4 * lax.rem(z + s, 2) + lax.rem(y + r, 4)

    def group(p):
        return {"blk": x * 8 + p}

    def along(o):
        return {"blk": lax.rem(x + o, 4) * 8 + me}

    def sibling(o):
        return {"table": lax.rem(tab + o, TABLE)}

    xp, xm = along(1), along(3)
    yp = group(slot(1, 0))
    ym = group(slot(3, 0))
    zp = group(slot(0, 1))

    own_q = pltpu.make_async_copy(q_hbm, qbuf.at[me], lsem.at[0])
    own_k = pltpu.make_async_copy(k_hbm, kbuf.at[0], lsem.at[1])
    own_q.start()
    own_k.start()

    barrier = pltpu.get_barrier_semaphore()
    peers = [group(lax.rem(me + o, 8)) for o in range(1, 8)]
    tables = [sibling(o) for o in range(1, TABLE)]
    for to in peers + [along(o) for o in range(1, 4)] + tables:
        pl.semaphore_signal(barrier, inc=1, device_id=to, device_id_type=MESH)
    pl.semaphore_wait(barrier, 13)
    for to in tables:
        pl.semaphore_signal(token.at[0], inc=1, device_id=to, device_id_type=MESH)
    own_k.wait()
    own_q.wait()

    def half(ref, i, c):
        return ref.at[i, pl.ds(c * H, H)]

    def send(n, src, dst, to):
        copy = pltpu.make_async_remote_copy(
            src_ref=src, dst_ref=dst, send_sem=ssem.at[n], recv_sem=rsem.at[n],
            device_id=to, device_id_type=MESH,
        )
        copy.start()
        return copy

    def arrived(n, ref):
        pltpu.make_async_remote_copy(
            src_ref=ref, dst_ref=ref, send_sem=ssem.at[n], recv_sem=rsem.at[n],
            device_id=xp, device_id_type=MESH,
        ).wait_recv()

    sent = []

    def k_send(n, i, j, c):
        sent.append(send(n, half(kbuf, i, c), half(kbuf, j, c), xp))

    def q_send(n, i, c, to):
        sent.append(send(n, half(qbuf, i, c), half(qbuf, i, c), to))

    k_send(0, 0, 1, 0)
    q_send(4, me, 0, yp)
    q_send(7, me, 1, ym)
    q_send(8, me, 0, zp)
    k_send(1, 0, 1, 1)
    q_send(5, me, 1, yp)
    q_send(6, me, 0, ym)
    q_send(9, me, 1, zp)

    def scores(qi, kind, ks):
        top = jnp.full((8, N), -jnp.inf, F32)
        for t in range(2):
            rows = pl.ds(t * H, H)
            s = lax.dot_general(kbuf[ks, rows, :], qbuf[qi], NT, preferred_element_type=F32)
            sbuf[kind, qi, rows, :] = s
            top = jnp.maximum(top, jnp.max(s.reshape(H // 8, 8, N), axis=0))
        top = jnp.max(top, axis=0, keepdims=True) * C2
        total = jnp.zeros((8, N), F32)
        for t in range(2):
            s = sbuf[kind, qi, pl.ds(t * H, H), :]
            total = total + jnp.sum(jnp.exp2(s * C2 - top).reshape(H // 8, 8, N), axis=0)
        total = jnp.sum(total, axis=0, keepdims=True)
        lk[kind, pl.ds(qi, 1), :] = top + jnp.log(total) * LOG2E

    def mixed_k(qi):
        return jnp.where(qi >= me, 0, 2)

    scores(me, 1, 0)

    owner = owner_ref[...]
    owner_f = owner.astype(F32)
    owner_col = jnp.broadcast_to(owner_f, (8, N)).T[:, 0:1]
    before = lax.broadcasted_iota(jnp.int32, (N, N), 0) < lax.broadcasted_iota(jnp.int32, (N, N), 1)
    rank = jnp.sum(jnp.where((owner_col == owner_f) & before, 1.0, 0.0), axis=0, keepdims=True)
    rank = rank.astype(jnp.int32)
    away = owner - b * TABLE
    away = jnp.where(away < 0, away + DEVS, away)
    keys[...] = away * (2 * CAP) + rank
    row = row_ref[...] + 1
    sub = lax.broadcasted_iota(jnp.int32, (DEVS, N), 0)
    mine = sub == away
    high = jnp.where(mine, (row // 128).astype(F32), 0.0).astype(BF16)
    low = jnp.where(mine, (row % 128).astype(F32), 0.0).astype(BF16)
    place = jnp.where(sub == rank, 1.0, 0.0).astype(BF16)
    message = 128.0 * lax.dot_general(high, place, NT, preferred_element_type=F32)
    message = message + lax.dot_general(low, place, NT, preferred_element_type=F32)
    ids[...] = message.astype(jnp.int32).reshape(DEVS, 1, 128)
    got_ids[dev] = ids[tab]

    def post(src, dst, n, o, t):
        pltpu.make_async_remote_copy(
            src_ref=src.at[o * TABLE + t], dst_ref=dst.at[dev], send_sem=ex_s.at[n], recv_sem=ex_r.at[n],
            device_id={"blk": lax.rem(b + o, BLK), "table": t}, device_id_type=MESH,
        ).start()

    def post_near(src, dst, n):
        for t in range(TABLE):

            @pl.when(tab != t)
            def _():
                post(src, dst, n, 0, t)

    def tell(o, carry):
        for t in range(TABLE):
            post(ids, got_ids, 0, o, t)
        return carry


    s3, s1, s2, s0 = slot(3, 0), slot(1, 0), slot(2, 0), slot(0, 1)
    t3, t1, t2 = slot(3, 1), slot(1, 1), slot(2, 1)
    arrived(0, half(kbuf, 1, 0))
    k_send(2, 1, 2, 0)
    arrived(4, half(qbuf, s3, 0))
    q_send(10, s3, 0, yp)
    arrived(7, half(qbuf, s1, 1))
    q_send(11, s1, 1, ym)
    arrived(8, half(qbuf, s0, 0))
    q_send(12, s0, 0, yp)
    q_send(14, s0, 0, ym)
    arrived(1, half(kbuf, 1, 1))
    k_send(3, 1, 2, 1)
    arrived(9, half(qbuf, s0, 1))
    q_send(13, s0, 1, yp)
    q_send(15, s0, 1, ym)
    pl.semaphore_wait(token.at[0], TABLE - 1)
    for to in peers:
        pl.semaphore_signal(token.at[1], inc=1, device_id=to, device_id_type=MESH)
    arrived(5, half(qbuf, s3, 1))
    arrived(6, half(qbuf, s1, 0))
    scores(me, 0, 1)

    def first_full(j, carry):
        scores(slot(j + lax.div(j, 2), lax.div(4 - j, 4)), 0, 1)
        return carry

    lax.fori_loop(0, 3, first_full, 0)
    arrived(10, half(qbuf, s2, 0))
    q_send(16, s2, 0, zp)
    arrived(11, half(qbuf, s2, 1))
    q_send(17, s2, 1, zp)
    scores(s2, 0, 1)
    arrived(2, half(kbuf, 2, 0))
    arrived(3, half(kbuf, 2, 1))

    def turn(i, carry):
        kt[i] = kbuf[i].T
        return carry

    lax.fori_loop(0, 3, turn, 0)

    def first_mixed(j, carry):
        qi = slot(j, (4 - j) // 4)
        scores(qi, 1, mixed_k(qi))
        return carry

    lax.fori_loop(0, 4, first_mixed, 0)
    pl.semaphore_wait(token.at[1], 7)
    post_near(ids, got_ids, 0)
    lax.fori_loop(1, 16, tell, 0)

    def last_pairs(r):
        qi = slot(r, 1)
        scores(qi, 0, 1)
        scores(qi, 1, mixed_k(qi))

    arrived(12, half(qbuf, t3, 0))
    arrived(13, half(qbuf, t3, 1))
    last_pairs(3)
    arrived(14, half(qbuf, t1, 0))
    arrived(15, half(qbuf, t1, 1))
    last_pairs(1)
    arrived(16, half(qbuf, t2, 0))
    arrived(17, half(qbuf, t2, 1))
    last_pairs(2)

    a, c = lk[0], lk[1]
    top = jnp.maximum(a, c)
    lst[me] = top + jnp.log(jnp.exp2(a - top) + jnp.exp2(c - top)) * LOG2E
    stats = []
    most = pl.ds(0, DEVS - 1)
    for o in range(1, 8):
        copy = pltpu.make_async_remote_copy(
            src_ref=lst.at[me], dst_ref=lst.at[me], send_sem=st_s.at[o - 1], recv_sem=st_r.at[o - 1],
            device_id=group(lax.rem(me + o, 8)), device_id_type=MESH,
        )
        copy.start()
        stats.append(copy)
    lax.fori_loop(16, BLK, tell, 0)

    for o in range(1, 8):
        p = lax.rem(me + 8 - o, 8)
        pltpu.make_async_remote_copy(
            src_ref=lst.at[p], dst_ref=lst.at[p], send_sem=st_s.at[o - 1], recv_sem=st_r.at[o - 1],
            device_id=xp, device_id_type=MESH,
        ).wait_recv()
    top = lst[0]
    for i in range(1, 8):
        top = jnp.maximum(top, lst[i])
    total = jnp.exp2(lst[0] - top)
    for i in range(1, 8):
        total = total + jnp.exp2(lst[i] - top)
    lse[...] = top + jnp.log(total) * LOG2E

    def item_rows(kind, qi, t, hot):
        w = jnp.exp2(sbuf[kind, qi, pl.ds(t * H, H), :] * C2 - lse[pl.ds(qi, 1), :])
        if hot:
            places = lax.broadcasted_iota(jnp.int32, (H, N), 0) + t * H
            w = jnp.where(places == pos_ref[...], w - 1.0, w)
        w = w.astype(BF16)
        gbuf[kind, qi, pl.ds(t * H, H), :] = w
        acc[pl.ds(t * H, H), :] += jnp.dot(w, qbuf[qi], preferred_element_type=F32)

    def items_of(kind, lo, hi):
        acc[...] = jnp.zeros((N, D), F32)

        def one(qi, carry):
            for t in range(2):
                item_rows(kind, qi, t, False)
            return carry

        lax.fori_loop(lo, hi, one, 0)

    items_of(1, 0, me)
    pk[0] = acc[...].astype(BF16)
    sent.append(send(18, half(pk, 0, 0), half(pr, 0, 0), xm))
    sent.append(send(19, half(pk, 0, 1), half(pr, 0, 1), xp))
    items_of(0, 0, 8)
    pk[1, pl.ds(H, H), :] = acc[pl.ds(H, H), :].astype(BF16)
    sent.append(send(21, half(pk, 1, 1), half(pr, 1, 1), xm))
    arrived(18, half(pr, 0, 0))
    pk[1, pl.ds(0, H), :] = (acc[pl.ds(0, H), :] + pr[0, pl.ds(0, H), :].astype(F32)).astype(BF16)
    sent.append(send(20, half(pk, 1, 0), half(pr, 1, 0), xm))
    arrived(19, half(pr, 0, 1))
    sent.append(send(22, half(pr, 0, 1), half(pr, 2, 1), xp))
    items_of(1, me + 1, 8)
    for t in range(2):
        item_rows(1, me, t, True)

    def query_part(qi):
        ks = mixed_k(qi)
        part = jnp.dot(kt[1], gbuf[0, qi], preferred_element_type=F32)
        return part + jnp.dot(kt[ks], gbuf[1, qi], preferred_element_type=F32)

    def give(i, h, value, to):
        tx[i, h] = value.astype(BF16)
        copy = pltpu.make_async_remote_copy(
            src_ref=tx.at[i, h], dst_ref=rx.at[i, h], send_sem=dq_s.at[2 * i + h],
            recv_sem=dq_r.at[2 * i + h], device_id=to, device_id_type=MESH,
        )
        copy.start()
        sent.append(copy)

    def given(i, h):
        pltpu.make_async_remote_copy(
            src_ref=rx.at[i, h], dst_ref=rx.at[i, h], send_sem=dq_s.at[2 * i + h],
            recv_sem=dq_r.at[2 * i + h], device_id=xp, device_id_type=MESH,
        ).wait_recv()
        return rx[i, h].astype(F32)

    for i, r, to in ((0, 2, zp), (4, 1, yp), (5, 3, ym)):
        part = query_part(slot(r, 1))
        give(i, 0, part[:, :H], to)
        give(i, 1, part[:, H:], to)
    part = query_part(slot(1, 0))
    give(2, 1, part[:, H:], yp)
    keep[0] = part[:, :H]
    part = query_part(slot(3, 0))
    give(3, 0, part[:, :H], ym)
    keep[1] = part[:, H:]
    part = query_part(slot(0, 1))
    keep[2] = part[:, :H]
    keep[3] = part[:, H:]
    part = query_part(slot(2, 0))
    keep[4] = part[:, :H]
    keep[5] = part[:, H:]
    part = query_part(me)
    keep[6] = part[:, :H]
    keep[7] = part[:, H:]
    give(1, 0, keep[4] + given(0, 0), yp)

    low, high = pl.ds(0, H), pl.ds(H, H)
    arrived(21, half(pr, 1, 1))
    arrived(22, half(pr, 2, 1))
    lower = acc[high, :] + pr[1, high, :].astype(F32) + pr[2, high, :].astype(F32)
    dk_ref[high, :] = (SCALE * lower).astype(BF16)
    arrived(20, half(pr, 1, 0))
    dk_ref[low, :] = (SCALE * (acc[low, :] + pr[1, low, :].astype(F32))).astype(BF16)
    give(1, 1, keep[5] + given(0, 1), ym)

    own = pltpu.make_async_copy(rows_out.at[tab], got_ref.at[dev], lsem.at[2])

    def dispatch(g, carry):
        at = lax.broadcasted_iota(jnp.int32, (16 * 2 * CAP, N), 0) + g * (16 * 2 * CAP)
        left = jnp.where(at == keys[...], 1.0, 0.0).astype(BF16)
        right = jnp.where(at == keys[...] + CAP, 1.0, 0.0).astype(BF16)
        picked = jnp.dot(left, dk_ref[:, 0:128], preferred_element_type=F32)
        picked = picked + jnp.dot(right, dk_ref[:, 128:256], preferred_element_type=F32)
        rows_out[pl.ds(g * 16, 16)] = picked.astype(BF16).reshape(16, 2 * CAP, 128)

        @pl.when(g == 0)
        def _():
            own.start()
            post_near(rows_out, got_ref, 1)

        def four(j, c):
            for t in range(TABLE):
                post(rows_out, got_ref, 1, g * 4 + j, t)
            return c

        lax.fori_loop(jnp.where(g == 0, 1, 0), 4, four, 0)
        return carry

    lax.fori_loop(0, 8, dispatch, 0)

    for h in range(2):
        give(6, h, keep[2 + h] + given(4, h) + given(5, h), zp)
    give(2, 0, keep[0] + given(1, 0), yp)
    give(3, 1, keep[1] + given(1, 1), ym)

    tells = pltpu.make_async_remote_copy(
        src_ref=ids.at[most], dst_ref=got_ids.at[most], send_sem=ex_s.at[0], recv_sem=ex_r.at[0],
        device_id=xp, device_id_type=MESH,
    )
    tells.wait()
    listing(got_ids[...].reshape(DEVS, 128), meta_ref, posb, valb)

    for h in range(2):
        mine = keep[6 + h] + given(2, h) + given(3, h) + given(6, h)
        dq_ref[pl.ds(h * H, H), :] = (SCALE * mine).T.astype(BF16)

    own.wait()
    pltpu.make_async_remote_copy(
        src_ref=rows_out.at[most], dst_ref=got_ref.at[most], send_sem=ex_s.at[1],
        recv_sem=ex_r.at[1], device_id=xp, device_id_type=MESH,
    ).wait()
    for copy in sent:
        copy.wait_send()
    for copy in stats:
        copy.wait_send()


def main_call(queries, items, positives, owner, row):
    vmem = pl.BlockSpec(memory_space=pltpu.VMEM)
    hbm = pl.BlockSpec(memory_space=pl.ANY)
    dma = pltpu.SemaphoreType.DMA
    return pl.pallas_call(
        main_kernel,
        out_shape=(
            jax.ShapeDtypeStruct((N, D), BF16),
            jax.ShapeDtypeStruct((N, D), BF16),
            jax.ShapeDtypeStruct((DEVS, 2 * CAP, 128), BF16),
            jax.ShapeDtypeStruct((LIST + 1, 128), jnp.int32),
        ),
        in_specs=[hbm, hbm, vmem, vmem, vmem],
        out_specs=(vmem, vmem, hbm, vmem),
        scratch_shapes=[
            pltpu.VMEM((8, N, D), BF16),
            pltpu.VMEM((3, N, D), BF16),
            pltpu.VMEM((2, 8, N, N), F32),
            pltpu.VMEM((2, 8, N, N), BF16),
            pltpu.VMEM((3, D, N), BF16),
            pltpu.VMEM((2, 8, N), F32),
            pltpu.VMEM((8, 8, N), F32),
            pltpu.VMEM((8, N), F32),
            pltpu.VMEM((N, D), F32),
            pltpu.VMEM((2, N, D), BF16),
            pltpu.VMEM((3, N, D), BF16),
            pltpu.VMEM((7, 2, D, H), BF16),
            pltpu.VMEM((7, 2, D, H), BF16),
            pltpu.VMEM((8, D, H), F32),
            pltpu.VMEM((1, N), jnp.int32),
            pltpu.VMEM((DEVS, 1, 128), jnp.int32),
            pltpu.VMEM((DEVS, 1, 128), jnp.int32),
            pltpu.VMEM((DEVS, 2 * CAP, 128), BF16),
            pltpu.VMEM((CAP, DEVS, 128), jnp.int32),
            pltpu.VMEM((CAP, DEVS, 128), jnp.int32),
            dma((3,)), dma((23,)), dma((23,)), dma((7,)), dma((7,)), dma((14,)), dma((14,)),
            dma((2,)), dma((2,)), pltpu.SemaphoreType.REGULAR((2,)),
        ],
        compiler_params=pltpu.CompilerParams(
            collective_id=0, has_side_effects=True, vmem_limit_bytes=60 * 1024 * 1024
        ),
        name="band",
    )(queries, items, positives.reshape(1, N), owner.reshape(1, N), row.reshape(1, N))


PIECE = 1024
SLOTS = 8
STEP = 16


def table_kernel(
    meta, got_hbm, dq_in, dk_in, out, dq_out, dk_out, left, right, rows, stage, got, kept, sem, load_sem
):
    loads = [
        pltpu.make_async_copy(got_hbm, got, load_sem.at[0]),
        pltpu.make_async_copy(dq_in, kept.at[0], load_sem.at[1]),
        pltpu.make_async_copy(dk_in, kept.at[1], load_sem.at[2]),
    ]
    for copy in loads:
        copy.start()

    def clear(i, carry):
        to = pl.ds(pl.multiple_of(i * 512, 512), 512)
        left[to, :] = jnp.zeros((512, 128), F32)
        right[to, :] = jnp.zeros((512, 128), F32)
        return carry

    lax.fori_loop(0, ROWS_DEV // 512, clear, 0)
    for copy in loads:
        copy.wait()
    passed = [
        pltpu.make_async_copy(kept.at[0], dq_out, load_sem.at[3]),
        pltpu.make_async_copy(kept.at[1], dk_out, load_sem.at[4]),
    ]
    for copy in passed:
        copy.start()

    def widen(i, carry):
        to = pl.ds(pl.multiple_of(i * 384, 384), 384)
        rows[to, :] = got[pl.ds(i * 16, 16)].astype(F32).reshape(384, 128)
        return carry

    lax.fori_loop(0, DEVS // 16, widen, 0)

    def entry(n):
        v = meta[lax.shift_right_logical(n, 7), lax.bitwise_and(n, 127)]
        at = lax.shift_right_logical(v, 15)
        return pl.ds(lax.bitwise_and(v, 32767), 1), rows[pl.ds(at, 1), :], rows[pl.ds(at + CAP, 1), :]

    def place(i, carry):
        for to, a, b in [entry(i * STEP + j) for j in range(STEP)]:
            left[to, :] = a
            right[to, :] = b
        return carry

    lax.fori_loop(0, lax.div(meta[LIST, 0] + STEP - 1, STEP), place, 0)

    def again(i, carry):
        for j in range(STEP):
            to, a, b = entry(LIST * 128 - 1 - i * STEP - j)
            left[to, :] += a
            right[to, :] += b
        return carry

    lax.fori_loop(0, lax.div(meta[LIST, 1] + STEP - 1, STEP), again, 0)

    def piece(i):
        at = i * PIECE if isinstance(i, int) else pl.multiple_of(i * PIECE, PIECE)
        k = lax.rem(i, SLOTS)
        return pltpu.make_async_copy(stage.at[k], out.at[pl.ds(at, PIECE)], sem.at[k])

    def store(i, carry):
        @pl.when(i >= SLOTS)
        def _():
            piece(i - SLOTS).wait()

        k = lax.rem(i, SLOTS)

        def turn(j, c):
            at = pl.ds(pl.multiple_of(i * PIECE + j * 256, 256), 256)
            to = pl.ds(pl.multiple_of(j * 256, 256), 256)
            stage[k, to, 0:128] = left[at, :].astype(BF16)
            stage[k, to, 128:256] = right[at, :].astype(BF16)
            return c

        lax.fori_loop(0, PIECE // 256, turn, 0)
        piece(i).start()
        return carry

    pieces = ROWS_DEV // PIECE
    lax.fori_loop(0, pieces, store, 0)
    for i in range(pieces - SLOTS, pieces):
        piece(i).wait()
    for copy in passed:
        copy.wait()


def table_call(meta, got, query_grad, item_grad):
    hbm = pl.BlockSpec(memory_space=pl.ANY)
    grad = jax.ShapeDtypeStruct((N, D), BF16)
    return pl.pallas_call(
        table_kernel,
        out_shape=(jax.ShapeDtypeStruct((ROWS_DEV, D), BF16), grad, grad),
        in_specs=[pl.BlockSpec(memory_space=pltpu.SMEM), hbm, hbm, hbm],
        out_specs=(hbm, hbm, hbm),
        scratch_shapes=[
            pltpu.VMEM((ROWS_DEV + 8, 128), F32),
            pltpu.VMEM((ROWS_DEV + 8, 128), F32),
            pltpu.VMEM((DEVS * 2 * CAP, 128), F32),
            pltpu.VMEM((SLOTS, PIECE, D), BF16),
            pltpu.VMEM((DEVS, 2 * CAP, 128), BF16),
            pltpu.VMEM((2, N, D), BF16),
            pltpu.SemaphoreType.DMA((SLOTS,)),
            pltpu.SemaphoreType.DMA((5,)),
        ],
        compiler_params=pltpu.CompilerParams(vmem_limit_bytes=60 * 1024 * 1024),
        name="table",
    )(meta, got, query_grad, item_grad)


def local(queries, items, positives, item_owner, item_row):
    query_grad, item_grad, got, meta = main_call(queries, items, positives, item_owner, item_row)
    table_grad, query_grad, item_grad = table_call(meta, got, query_grad, item_grad)
    return (query_grad, item_grad, table_grad)


def solution(mesh):
    in_specs = (
        P(("blk", "table"), None),
        P(("blk", "table"), None),
        P(("blk", "table")),
        P(("blk", "table"), None),
        P(("blk", "table")),
    )
    out_specs = (P(("blk", "table"), None), P(("blk", "table"), None), P(("blk", "table"), None))
    return jax.shard_map(local, mesh=mesh, in_specs=in_specs, out_specs=out_specs, check_vma=False)
```

```python
import math

import jax
import jax.numpy as jnp
from jax import lax
from jax.experimental import pallas as pl
from jax.experimental.pallas import tpu as pltpu
from jax.sharding import PartitionSpec as P

ROWS_DEV = 16384
N = 512
D = 256
H = 256
DEVS = 128
TABLE = 4
CAP = 12
BLK = 32
LIST = 13
SCALE = 3.0 / math.sqrt(D)
LOG2E = 1.4426950408889634
C2 = SCALE * LOG2E
MESH = pl.DeviceIdType.MESH
NT = (((1,), (1,)), ((), ()))
F32 = jnp.float32
BF16 = jnp.bfloat16


def listing(got, meta_ref, posb, valb):
    lane = lax.broadcasted_iota(jnp.int32, (DEVS, 128), 1)
    subl = lax.broadcasted_iota(jnp.int32, (DEVS, 128), 0)
    ident = got.astype(F32)
    turned = ident.T
    number = turned.astype(jnp.int32) - 1
    high = lax.shift_right_arithmetic(number, 7)
    low = lax.bitwise_and(number, 127)

    def hot(which, c):
        return jnp.where(subl == which[c : c + 1, :], 1.0, 0.0)

    counts = jnp.zeros((DEVS, 128), F32)
    for c in range(CAP):
        counts = counts + lax.dot_general(
            hot(low, c).astype(BF16), hot(high, c).astype(BF16), NT, preferred_element_type=F32
        )
    counts = counts.astype(BF16)
    named = jnp.zeros((DEVS, 128), F32)
    for c in range(CAP):
        by_low = jnp.dot(counts, hot(high, c).astype(BF16), preferred_element_type=F32)
        times = jnp.sum(by_low * hot(low, c), axis=0, keepdims=True)
        named = jnp.where(subl == c, times, named)
    named = named.T
    first = jnp.where(named == 1.0, 1.0, 0.0).astype(BF16)
    again = jnp.where(named > 1.0, 1.0, 0.0).astype(BF16)
    upper = jnp.where(subl < lane, 1.0, 0.0).astype(BF16)
    lower = jnp.where(lane < subl, 1.0, 0.0).astype(BF16)
    ones = jnp.ones((DEVS, 128), BF16)

    def ranked(flags):
        per_row = jnp.dot(flags, ones, preferred_element_type=F32)
        place = jnp.dot(lower, per_row.astype(BF16), preferred_element_type=F32)
        place = place + jnp.dot(flags, upper, preferred_element_type=F32)
        return place.astype(jnp.int32), jnp.sum(per_row, axis=0, keepdims=True).astype(jnp.int32)

    first_at, first_count = ranked(first)
    again_at, again_count = ranked(again)
    pos = jnp.where(first > 0, first_at, jnp.where(again > 0, LIST * 128 - 1 - again_at, -1))
    value = got + 32768 * (subl * (2 * CAP) + lane)
    for c in range(CAP):
        posb[c] = jnp.broadcast_to(pos[:, c : c + 1], (DEVS, 128))
        valb[c] = jnp.broadcast_to(value[:, c : c + 1], (DEVS, 128))

    def listed(t, carry):
        at = lane + t * 128
        found = jnp.zeros((8, 128), jnp.int32)
        for c in range(CAP):
            hit = jnp.where(posb[c] == at, valb[c], 0)
            found = found + jnp.sum(hit.reshape(DEVS // 8, 8, 128), axis=0)
        found = jnp.sum(found, axis=0, keepdims=True)
        meta_ref[pl.ds(t, 1), :] = jnp.where(found > 0, found - 1, ROWS_DEV)
        return carry

    lax.fori_loop(0, LIST, listed, 0)
    one = lax.broadcasted_iota(jnp.int32, (1, 128), 1)
    meta_ref[pl.ds(LIST, 1), :] = jnp.where(one == 0, first_count, again_count)


def main_kernel(
    q_hbm, k_hbm, pos_ref, owner_ref, row_ref,
    dq_ref, dk_ref, got_ref, meta_ref,
    qbuf, kbuf, sbuf, gbuf, kt, lk, lst, lse, acc, pk, pr, tx, rx, keep,
    keys, ids, got_ids, rows_out, posb, valb,
    lsem, ssem, rsem, st_s, st_r, dq_s, dq_r, ex_s, ex_r, token,
):
    b = lax.axis_index("blk")
    tab = lax.axis_index("table")
    x = lax.div(b, 8)
    me = lax.rem(b, 8)
    z = lax.div(me, 4)
    y = lax.rem(me, 4)
    dev = b * TABLE + tab

    def slot(r, s):
        return 4 * lax.rem(z + s, 2) + lax.rem(y + r, 4)

    def group(p):
        return {"blk": x * 8 + p}

    def along(o):
        return {"blk": lax.rem(x + o, 4) * 8 + me}

    def sibling(o):
        return {"table": lax.rem(tab + o, TABLE)}

    xp, xm = along(1), along(3)
    yp = group(slot(1, 0))
    ym = group(slot(3, 0))
    zp = group(slot(0, 1))

    own_q = pltpu.make_async_copy(q_hbm, qbuf.at[me], lsem.at[0])
    own_k = pltpu.make_async_copy(k_hbm, kbuf.at[0], lsem.at[1])
    own_q.start()
    own_k.start()

    barrier = pltpu.get_barrier_semaphore()
    peers = [group(lax.rem(me + o, 8)) for o in range(1, 8)]
    tables = [sibling(o) for o in range(1, TABLE)]
    for to in peers + [along(o) for o in range(1, 4)] + tables:
        pl.semaphore_signal(barrier, inc=1, device_id=to, device_id_type=MESH)
    pl.semaphore_wait(barrier, 13)
    for to in tables:
        pl.semaphore_signal(token.at[0], inc=1, device_id=to, device_id_type=MESH)
    own_k.wait()
    own_q.wait()

    def half(ref, i, c):
        return ref.at[i, pl.ds(c * H, H)]

    def send(n, src, dst, to):
        copy = pltpu.make_async_remote_copy(
            src_ref=src, dst_ref=dst, send_sem=ssem.at[n], recv_sem=rsem.at[n],
            device_id=to, device_id_type=MESH,
        )
        copy.start()
        return copy

    def arrived(n, ref):
        pltpu.make_async_remote_copy(
            src_ref=ref, dst_ref=ref, send_sem=ssem.at[n], recv_sem=rsem.at[n],
            device_id=xp, device_id_type=MESH,
        ).wait_recv()

    sent = []

    def k_send(n, i, j, c):
        sent.append(send(n, half(kbuf, i, c), half(kbuf, j, c), xp))

    def q_send(n, i, c, to):
        sent.append(send(n, half(qbuf, i, c), half(qbuf, i, c), to))

    k_send(0, 0, 1, 0)
    q_send(4, me, 0, yp)
    q_send(7, me, 1, ym)
    q_send(8, me, 0, zp)
    k_send(1, 0, 1, 1)
    q_send(5, me, 1, yp)
    q_send(6, me, 0, ym)
    q_send(9, me, 1, zp)

    def scores(qi, kind, ks):
        top = jnp.full((8, N), -jnp.inf, F32)
        for t in range(2):
            rows = pl.ds(t * H, H)
            s = lax.dot_general(kbuf[ks, rows, :], qbuf[qi], NT, preferred_element_type=F32)
            sbuf[kind, qi, rows, :] = s
            top = jnp.maximum(top, jnp.max(s.reshape(H // 8, 8, N), axis=0))
        top = jnp.max(top, axis=0, keepdims=True) * C2
        total = jnp.zeros((8, N), F32)
        for t in range(2):
            s = sbuf[kind, qi, pl.ds(t * H, H), :]
            total = total + jnp.sum(jnp.exp2(s * C2 - top).reshape(H // 8, 8, N), axis=0)
        total = jnp.sum(total, axis=0, keepdims=True)
        lk[kind, pl.ds(qi, 1), :] = top + jnp.log(total) * LOG2E

    def mixed_k(qi):
        return jnp.where(qi >= me, 0, 2)

    scores(me, 1, 0)

    owner = owner_ref[...]
    owner_f = owner.astype(F32)
    owner_col = jnp.broadcast_to(owner_f, (8, N)).T[:, 0:1]
    before = lax.broadcasted_iota(jnp.int32, (N, N), 0) < lax.broadcasted_iota(jnp.int32, (N, N), 1)
    rank = jnp.sum(jnp.where((owner_col == owner_f) & before, 1.0, 0.0), axis=0, keepdims=True)
    rank = rank.astype(jnp.int32)
    away = owner - b * TABLE
    away = jnp.where(away < 0, away + DEVS, away)
    keys[...] = away * (2 * CAP) + rank
    row = row_ref[...] + 1
    sub = lax.broadcasted_iota(jnp.int32, (DEVS, N), 0)
    mine = sub == away
    high = jnp.where(mine, (row // 128).astype(F32), 0.0).astype(BF16)
    low = jnp.where(mine, (row % 128).astype(F32), 0.0).astype(BF16)
    place = jnp.where(sub == rank, 1.0, 0.0).astype(BF16)
    message = 128.0 * lax.dot_general(high, place, NT, preferred_element_type=F32)
    message = message + lax.dot_general(low, place, NT, preferred_element_type=F32)
    ids[...] = message.astype(jnp.int32).reshape(DEVS, 1, 128)
    got_ids[dev] = ids[tab]

    def post(src, dst, n, o, t):
        pltpu.make_async_remote_copy(
            src_ref=src.at[o * TABLE + t], dst_ref=dst.at[dev], send_sem=ex_s.at[n], recv_sem=ex_r.at[n],
            device_id={"blk": lax.rem(b + o, BLK), "table": t}, device_id_type=MESH,
        ).start()

    def post_near(src, dst, n):
        for t in range(TABLE):

            @pl.when(tab != t)
            def _():
                post(src, dst, n, 0, t)

    def tell(o, carry):
        for t in range(TABLE):
            post(ids, got_ids, 0, o, t)
        return carry


    s3, s1, s2, s0 = slot(3, 0), slot(1, 0), slot(2, 0), slot(0, 1)
    t3, t1, t2 = slot(3, 1), slot(1, 1), slot(2, 1)
    arrived(0, half(kbuf, 1, 0))
    k_send(2, 1, 2, 0)
    arrived(4, half(qbuf, s3, 0))
    q_send(10, s3, 0, yp)
    arrived(7, half(qbuf, s1, 1))
    q_send(11, s1, 1, ym)
    arrived(8, half(qbuf, s0, 0))
    q_send(12, s0, 0, yp)
    q_send(14, s0, 0, ym)
    arrived(1, half(kbuf, 1, 1))
    k_send(3, 1, 2, 1)
    arrived(9, half(qbuf, s0, 1))
    q_send(13, s0, 1, yp)
    q_send(15, s0, 1, ym)
    pl.semaphore_wait(token.at[0], TABLE - 1)
    for to in peers:
        pl.semaphore_signal(token.at[1], inc=1, device_id=to, device_id_type=MESH)
    arrived(5, half(qbuf, s3, 1))
    arrived(6, half(qbuf, s1, 0))
    scores(me, 0, 1)

    def first_full(j, carry):
        scores(slot(j + lax.div(j, 2), lax.div(4 - j, 4)), 0, 1)
        return carry

    lax.fori_loop(0, 3, first_full, 0)
    arrived(10, half(qbuf, s2, 0))
    q_send(16, s2, 0, zp)
    arrived(11, half(qbuf, s2, 1))
    q_send(17, s2, 1, zp)
    scores(s2, 0, 1)
    arrived(2, half(kbuf, 2, 0))
    arrived(3, half(kbuf, 2, 1))

    def turn(i, carry):
        kt[i] = kbuf[i].T
        return carry

    lax.fori_loop(0, 3, turn, 0)

    def first_mixed(j, carry):
        qi = slot(j, (4 - j) // 4)
        scores(qi, 1, mixed_k(qi))
        return carry

    lax.fori_loop(0, 4, first_mixed, 0)
    pl.semaphore_wait(token.at[1], 7)
    post_near(ids, got_ids, 0)
    lax.fori_loop(1, 16, tell, 0)

    def last_pairs(r):
        qi = slot(r, 1)
        scores(qi, 0, 1)
        scores(qi, 1, mixed_k(qi))

    arrived(12, half(qbuf, t3, 0))
    arrived(13, half(qbuf, t3, 1))
    last_pairs(3)
    arrived(14, half(qbuf, t1, 0))
    arrived(15, half(qbuf, t1, 1))
    last_pairs(1)
    arrived(16, half(qbuf, t2, 0))
    arrived(17, half(qbuf, t2, 1))
    last_pairs(2)

    a, c = lk[0], lk[1]
    top = jnp.maximum(a, c)
    lst[me] = top + jnp.log(jnp.exp2(a - top) + jnp.exp2(c - top)) * LOG2E
    stats = []
    most = pl.ds(0, DEVS - 1)
    for o in range(1, 8):
        copy = pltpu.make_async_remote_copy(
            src_ref=lst.at[me], dst_ref=lst.at[me], send_sem=st_s.at[o - 1], recv_sem=st_r.at[o - 1],
            device_id=group(lax.rem(me + o, 8)), device_id_type=MESH,
        )
        copy.start()
        stats.append(copy)
    lax.fori_loop(16, BLK, tell, 0)

    for o in range(1, 8):
        p = lax.rem(me + 8 - o, 8)
        pltpu.make_async_remote_copy(
            src_ref=lst.at[p], dst_ref=lst.at[p], send_sem=st_s.at[o - 1], recv_sem=st_r.at[o - 1],
            device_id=xp, device_id_type=MESH,
        ).wait_recv()
    top = lst[0]
    for i in range(1, 8):
        top = jnp.maximum(top, lst[i])
    total = jnp.exp2(lst[0] - top)
    for i in range(1, 8):
        total = total + jnp.exp2(lst[i] - top)
    lse[...] = top + jnp.log(total) * LOG2E

    def item_rows(kind, qi, t, hot):
        w = jnp.exp2(sbuf[kind, qi, pl.ds(t * H, H), :] * C2 - lse[pl.ds(qi, 1), :])
        if hot:
            places = lax.broadcasted_iota(jnp.int32, (H, N), 0) + t * H
            w = jnp.where(places == pos_ref[...], w - 1.0, w)
        w = w.astype(BF16)
        gbuf[kind, qi, pl.ds(t * H, H), :] = w
        acc[pl.ds(t * H, H), :] += jnp.dot(w, qbuf[qi], preferred_element_type=F32)

    def items_of(kind, lo, hi):
        acc[...] = jnp.zeros((N, D), F32)

        def one(qi, carry):
            for t in range(2):
                item_rows(kind, qi, t, False)
            return carry

        lax.fori_loop(lo, hi, one, 0)

    items_of(1, 0, me)
    pk[0] = acc[...].astype(BF16)
    sent.append(send(18, half(pk, 0, 0), half(pr, 0, 0), xm))
    sent.append(send(19, half(pk, 0, 1), half(pr, 0, 1), xp))
    items_of(0, 0, 8)
    pk[1, pl.ds(H, H), :] = acc[pl.ds(H, H), :].astype(BF16)
    sent.append(send(21, half(pk, 1, 1), half(pr, 1, 1), xm))
    arrived(18, half(pr, 0, 0))
    pk[1, pl.ds(0, H), :] = (acc[pl.ds(0, H), :] + pr[0, pl.ds(0, H), :].astype(F32)).astype(BF16)
    sent.append(send(20, half(pk, 1, 0), half(pr, 1, 0), xm))
    arrived(19, half(pr, 0, 1))
    sent.append(send(22, half(pr, 0, 1), half(pr, 2, 1), xp))
    items_of(1, me + 1, 8)
    for t in range(2):
        item_rows(1, me, t, True)

    def query_part(qi):
        ks = mixed_k(qi)
        part = jnp.dot(kt[1], gbuf[0, qi], preferred_element_type=F32)
        return part + jnp.dot(kt[ks], gbuf[1, qi], preferred_element_type=F32)

    def give(i, h, value, to):
        tx[i, h] = value.astype(BF16)
        copy = pltpu.make_async_remote_copy(
            src_ref=tx.at[i, h], dst_ref=rx.at[i, h], send_sem=dq_s.at[2 * i + h],
            recv_sem=dq_r.at[2 * i + h], device_id=to, device_id_type=MESH,
        )
        copy.start()
        sent.append(copy)

    def given(i, h):
        pltpu.make_async_remote_copy(
            src_ref=rx.at[i, h], dst_ref=rx.at[i, h], send_sem=dq_s.at[2 * i + h],
            recv_sem=dq_r.at[2 * i + h], device_id=xp, device_id_type=MESH,
        ).wait_recv()
        return rx[i, h].astype(F32)

    for i, r, to in ((0, 2, zp), (4, 1, yp), (5, 3, ym)):
        part = query_part(slot(r, 1))
        give(i, 0, part[:, :H], to)
        give(i, 1, part[:, H:], to)
    part = query_part(slot(1, 0))
    give(2, 1, part[:, H:], yp)
    keep[0] = part[:, :H]
    part = query_part(slot(3, 0))
    give(3, 0, part[:, :H], ym)
    keep[1] = part[:, H:]
    part = query_part(slot(0, 1))
    keep[2] = part[:, :H]
    keep[3] = part[:, H:]
    part = query_part(slot(2, 0))
    keep[4] = part[:, :H]
    keep[5] = part[:, H:]
    part = query_part(me)
    keep[6] = part[:, :H]
    keep[7] = part[:, H:]
    give(1, 0, keep[4] + given(0, 0), yp)

    low, high = pl.ds(0, H), pl.ds(H, H)
    arrived(21, half(pr, 1, 1))
    arrived(22, half(pr, 2, 1))
    lower = acc[high, :] + pr[1, high, :].astype(F32) + pr[2, high, :].astype(F32)
    dk_ref[high, :] = (SCALE * lower).astype(BF16)
    arrived(20, half(pr, 1, 0))
    dk_ref[low, :] = (SCALE * (acc[low, :] + pr[1, low, :].astype(F32))).astype(BF16)
    give(1, 1, keep[5] + given(0, 1), ym)

    own = pltpu.make_async_copy(rows_out.at[tab], got_ref.at[dev], lsem.at[2])

    def dispatch(g, carry):
        at = lax.broadcasted_iota(jnp.int32, (16 * 2 * CAP, N), 0) + g * (16 * 2 * CAP)
        left = jnp.where(at == keys[...], 1.0, 0.0).astype(BF16)
        right = jnp.where(at == keys[...] + CAP, 1.0, 0.0).astype(BF16)
        picked = jnp.dot(left, dk_ref[:, 0:128], preferred_element_type=F32)
        picked = picked + jnp.dot(right, dk_ref[:, 128:256], preferred_element_type=F32)
        rows_out[pl.ds(g * 16, 16)] = picked.astype(BF16).reshape(16, 2 * CAP, 128)

        @pl.when(g == 0)
        def _():
            own.start()
            post_near(rows_out, got_ref, 1)

        def four(j, c):
            for t in range(TABLE):
                post(rows_out, got_ref, 1, g * 4 + j, t)
            return c

        lax.fori_loop(jnp.where(g == 0, 1, 0), 4, four, 0)
        return carry

    lax.fori_loop(0, 2, dispatch, 0)
    for h in range(2):
        give(6, h, keep[2 + h] + given(4, h) + given(5, h), zp)
    lax.fori_loop(2, 4, dispatch, 0)
    give(2, 0, keep[0] + given(1, 0), yp)
    give(3, 1, keep[1] + given(1, 1), ym)
    lax.fori_loop(4, 8, dispatch, 0)


    tells = pltpu.make_async_remote_copy(
        src_ref=ids.at[most], dst_ref=got_ids.at[most], send_sem=ex_s.at[0], recv_sem=ex_r.at[0],
        device_id=xp, device_id_type=MESH,
    )
    tells.wait()
    listing(got_ids[...].reshape(DEVS, 128), meta_ref, posb, valb)

    for h in range(2):
        mine = keep[6 + h] + given(2, h) + given(3, h) + given(6, h)
        dq_ref[pl.ds(h * H, H), :] = (SCALE * mine).T.astype(BF16)

    own.wait()
    pltpu.make_async_remote_copy(
        src_ref=rows_out.at[most], dst_ref=got_ref.at[most], send_sem=ex_s.at[1],
        recv_sem=ex_r.at[1], device_id=xp, device_id_type=MESH,
    ).wait()
    for copy in sent:
        copy.wait_send()
    for copy in stats:
        copy.wait_send()


def main_call(queries, items, positives, owner, row):
    vmem = pl.BlockSpec(memory_space=pltpu.VMEM)
    hbm = pl.BlockSpec(memory_space=pl.ANY)
    dma = pltpu.SemaphoreType.DMA
    return pl.pallas_call(
        main_kernel,
        out_shape=(
            jax.ShapeDtypeStruct((N, D), BF16),
            jax.ShapeDtypeStruct((N, D), BF16),
            jax.ShapeDtypeStruct((DEVS, 2 * CAP, 128), BF16),
            jax.ShapeDtypeStruct((LIST + 1, 128), jnp.int32),
        ),
        in_specs=[hbm, hbm, vmem, vmem, vmem],
        out_specs=(vmem, vmem, hbm, vmem),
        scratch_shapes=[
            pltpu.VMEM((8, N, D), BF16),
            pltpu.VMEM((3, N, D), BF16),
            pltpu.VMEM((2, 8, N, N), F32),
            pltpu.VMEM((2, 8, N, N), BF16),
            pltpu.VMEM((3, D, N), BF16),
            pltpu.VMEM((2, 8, N), F32),
            pltpu.VMEM((8, 8, N), F32),
            pltpu.VMEM((8, N), F32),
            pltpu.VMEM((N, D), F32),
            pltpu.VMEM((2, N, D), BF16),
            pltpu.VMEM((3, N, D), BF16),
            pltpu.VMEM((7, 2, D, H), BF16),
            pltpu.VMEM((7, 2, D, H), BF16),
            pltpu.VMEM((8, D, H), F32),
            pltpu.VMEM((1, N), jnp.int32),
            pltpu.VMEM((DEVS, 1, 128), jnp.int32),
            pltpu.VMEM((DEVS, 1, 128), jnp.int32),
            pltpu.VMEM((DEVS, 2 * CAP, 128), BF16),
            pltpu.VMEM((CAP, DEVS, 128), jnp.int32),
            pltpu.VMEM((CAP, DEVS, 128), jnp.int32),
            dma((3,)), dma((23,)), dma((23,)), dma((7,)), dma((7,)), dma((14,)), dma((14,)),
            dma((2,)), dma((2,)), pltpu.SemaphoreType.REGULAR((2,)),
        ],
        compiler_params=pltpu.CompilerParams(
            collective_id=0, has_side_effects=True, vmem_limit_bytes=60 * 1024 * 1024
        ),
        name="band",
    )(queries, items, positives.reshape(1, N), owner.reshape(1, N), row.reshape(1, N))


PIECE = 1024
SLOTS = 8
STEP = 16


def table_kernel(
    meta, got_hbm, dq_in, dk_in, out, dq_out, dk_out, left, right, rows, stage, got, kept, sem, load_sem
):
    loads = [
        pltpu.make_async_copy(got_hbm, got, load_sem.at[0]),
        pltpu.make_async_copy(dq_in, kept.at[0], load_sem.at[1]),
        pltpu.make_async_copy(dk_in, kept.at[1], load_sem.at[2]),
    ]
    for copy in loads:
        copy.start()

    def clear(i, carry):
        to = pl.ds(pl.multiple_of(i * 512, 512), 512)
        left[to, :] = jnp.zeros((512, 128), F32)
        right[to, :] = jnp.zeros((512, 128), F32)
        return carry

    lax.fori_loop(0, ROWS_DEV // 512, clear, 0)
    for copy in loads:
        copy.wait()
    passed = [
        pltpu.make_async_copy(kept.at[0], dq_out, load_sem.at[3]),
        pltpu.make_async_copy(kept.at[1], dk_out, load_sem.at[4]),
    ]
    for copy in passed:
        copy.start()

    def widen(i, carry):
        to = pl.ds(pl.multiple_of(i * 384, 384), 384)
        rows[to, :] = got[pl.ds(i * 16, 16)].astype(F32).reshape(384, 128)
        return carry

    lax.fori_loop(0, DEVS // 16, widen, 0)

    def entry(n):
        v = meta[lax.shift_right_logical(n, 7), lax.bitwise_and(n, 127)]
        at = lax.shift_right_logical(v, 15)
        return pl.ds(lax.bitwise_and(v, 32767), 1), rows[pl.ds(at, 1), :], rows[pl.ds(at + CAP, 1), :]

    def place(i, carry):
        for to, a, b in [entry(i * STEP + j) for j in range(STEP)]:
            left[to, :] = a
            right[to, :] = b
        return carry

    lax.fori_loop(0, lax.div(meta[LIST, 0] + STEP - 1, STEP), place, 0)

    def again(i, carry):
        for j in range(STEP):
            to, a, b = entry(LIST * 128 - 1 - i * STEP - j)
            left[to, :] += a
            right[to, :] += b
        return carry

    lax.fori_loop(0, lax.div(meta[LIST, 1] + STEP - 1, STEP), again, 0)

    def piece(i):
        at = i * PIECE if isinstance(i, int) else pl.multiple_of(i * PIECE, PIECE)
        k = lax.rem(i, SLOTS)
        return pltpu.make_async_copy(stage.at[k], out.at[pl.ds(at, PIECE)], sem.at[k])

    def store(i, carry):
        @pl.when(i >= SLOTS)
        def _():
            piece(i - SLOTS).wait()

        k = lax.rem(i, SLOTS)

        def turn(j, c):
            at = pl.ds(pl.multiple_of(i * PIECE + j * 256, 256), 256)
            to = pl.ds(pl.multiple_of(j * 256, 256), 256)
            stage[k, to, 0:128] = left[at, :].astype(BF16)
            stage[k, to, 128:256] = right[at, :].astype(BF16)
            return c

        lax.fori_loop(0, PIECE // 256, turn, 0)
        piece(i).start()
        return carry

    pieces = ROWS_DEV // PIECE
    lax.fori_loop(0, pieces, store, 0)
    for i in range(pieces - SLOTS, pieces):
        piece(i).wait()
    for copy in passed:
        copy.wait()


def table_call(meta, got, query_grad, item_grad):
    hbm = pl.BlockSpec(memory_space=pl.ANY)
    grad = jax.ShapeDtypeStruct((N, D), BF16)
    return pl.pallas_call(
        table_kernel,
        out_shape=(jax.ShapeDtypeStruct((ROWS_DEV, D), BF16), grad, grad),
        in_specs=[pl.BlockSpec(memory_space=pltpu.SMEM), hbm, hbm, hbm],
        out_specs=(hbm, hbm, hbm),
        scratch_shapes=[
            pltpu.VMEM((ROWS_DEV + 8, 128), F32),
            pltpu.VMEM((ROWS_DEV + 8, 128), F32),
            pltpu.VMEM((DEVS * 2 * CAP, 128), F32),
            pltpu.VMEM((SLOTS, PIECE, D), BF16),
            pltpu.VMEM((DEVS, 2 * CAP, 128), BF16),
            pltpu.VMEM((2, N, D), BF16),
            pltpu.SemaphoreType.DMA((SLOTS,)),
            pltpu.SemaphoreType.DMA((5,)),
        ],
        compiler_params=pltpu.CompilerParams(vmem_limit_bytes=60 * 1024 * 1024),
        name="table",
    )(meta, got, query_grad, item_grad)


def local(queries, items, positives, item_owner, item_row):
    query_grad, item_grad, got, meta = main_call(queries, items, positives, item_owner, item_row)
    table_grad, query_grad, item_grad = table_call(meta, got, query_grad, item_grad)
    return (query_grad, item_grad, table_grad)


def solution(mesh):
    in_specs = (
        P(("blk", "table"), None),
        P(("blk", "table"), None),
        P(("blk", "table")),
        P(("blk", "table"), None),
        P(("blk", "table")),
    )
    out_specs = (P(("blk", "table"), None), P(("blk", "table"), None), P(("blk", "table"), None))
    return jax.shard_map(local, mesh=mesh, in_specs=in_specs, out_specs=out_specs, check_vma=False)
```
